256 devices in a mesh: tables: 16 (over z_hi, y), cells: 16 (over z_lo, x, core).
Axes of the slice: x: 4, y: 4, z: 8 (z_hi: 4, z_lo: 2; z = z_hi * 2 + z_lo), core: 2. Of those that a mesh axis runs over, the one named last changes fastest.
Arguments:
- cells_in: bfloat16 [16, 512, 112, 192], P('tables', 'cells'), may hold values from -6 to 6
- train_count: int32 [16], P('tables'), may hold values from 128 to 384
- feat_count: int32 [16], P('tables'), may hold values from 28 to 112
- feat_qkv: bfloat16 [192, 576], replicated, may hold values from -2 to 2
- feat_proj: bfloat16 [192, 192], replicated, may hold values from -2 to 2
- row_qkv: bfloat16 [192, 576], replicated, may hold values from -2 to 2
- row_proj: bfloat16 [192, 192], replicated, may hold values from -0.4375 to 0.4375
- w_in: bfloat16 [192, 768], replicated, may hold values from -0.4375 to 0.4375
- w_out: bfloat16 [768, 192], replicated, may hold values from -0.21875 to 0.21875
- cotangent: bfloat16 [16, 512, 112, 192], P('tables', 'cells'), may hold values from -6 to 6
Outputs:
- cells_out: bfloat16 [16, 512, 112, 192], P('tables', 'cells')
- grad_in: float32 [192, 768], P(None, ('tables', 'cells'))
- grad_out: float32 [768, 192], P(('tables', 'cells'))
The draws below stay inside these ranges and needn't reach their ends.
All inputs are finite; a program needn't handle non-finite values.
Results may differ from the reference program's by a relative error of at most 0.018.
Values may be sent and summed in bfloat16 or wider, within the bound.
A program may use at most 128 MiB of HBM per device.

```python
import math
import jax
import jax.numpy as jnp
from jax import lax

E = 192
HEADS = 6
HEAD_DIM = 32
HID = 768
FEATS = 112
ROWS = 512
TABLES = 16


def base_weight(key, salt, rows, cols):
    values = jax.random.truncated_normal(jax.random.fold_in(key, salt), -6.0, 6.0, (rows, cols), jnp.float32)
    return values / jnp.float32(math.sqrt(rows))


def draw_feat_qkv(key, part):
    weight = base_weight(key, 31, E, 3 * E)
    return jnp.clip(weight, -2.0, 2.0).astype(jnp.bfloat16)


def draw_row_qkv(key, part):
    weight = base_weight(key, 41, E, 3 * E)
    return jnp.clip(weight, -2.0, 2.0).astype(jnp.bfloat16)


def draw_feat_proj(key, part):
    weight = base_weight(key, 51, E, E)
    return jnp.clip(weight, -2.0, 2.0).astype(jnp.bfloat16)


def draw_cells_in(key, part):
    cells = jax.random.truncated_normal(jax.random.fold_in(key, 21), -6.0, 6.0, (TABLES, ROWS, FEATS, E), jnp.float32)
    return jnp.clip(cells, -6.0, 6.0).astype(jnp.bfloat16)


def touch_ends(result, own_key, smallest, top_value):
    longest = result.shape.index(max(result.shape))
    spots = []
    for shift in (0, 1):
        where = [jax.random.randint(jax.random.fold_in(own_key, axis), (), 0, length) for axis, length in enumerate(result.shape)]
        where[longest] = (where[longest] + shift) % result.shape[longest]
        spots.append(tuple(where))
    return result.at[spots[0]].set(smallest).at[spots[1]].set(top_value)


def steps_of(own_key, shape, cuts, least, largest):
    loudness = 1.0
    for axis_at, shards_of in cuts:
        draws = jax.random.uniform(jax.random.fold_in(jax.random.fold_in(own_key, 6), axis_at), (shards_of,), jnp.float32, least / len(cuts), largest / len(cuts))
        loudness = loudness * jnp.repeat(jnp.exp(draws), shape[axis_at] // shards_of).reshape((-1,) + (1,) * (len(shape) - 1 - axis_at))
    return loudness


def bell_draw(rng, shape, scale, most, shards=(), kind=jnp.bfloat16):
    level = steps_of(rng, shape, shards, -0.22, 0.18) if shards else 1.0
    array = jax.random.normal(rng, shape, jnp.float32) * scale * level
    return jnp.minimum(jnp.maximum(array, -most), most).astype(kind)


def setup_inputs(seed: int = 0) -> dict:
    streams_of = jax.random.split(jax.random.key(seed), 11)
    cells_in = draw_cells_in(jax.random.fold_in(streams_of[10], 71), 0)
    train_count = touch_ends(jax.random.randint(streams_of[1], (TABLES,), ROWS // 4, ROWS - ROWS // 4 + 1), jax.random.fold_in(streams_of[1], 1), ROWS // 4, (ROWS - ROWS // 4 + 1) - 1).astype(jnp.int32)
    feat_count = touch_ends(jax.random.randint(streams_of[2], (TABLES,), FEATS // 4, FEATS + 1), jax.random.fold_in(streams_of[2], 1), FEATS // 4, FEATS).astype(jnp.int32)
    feat_qkv = draw_feat_qkv(jax.random.fold_in(streams_of[10], 71), 0)
    feat_proj = draw_feat_proj(jax.random.fold_in(streams_of[10], 71), 0)
    row_qkv = draw_row_qkv(jax.random.fold_in(streams_of[10], 71), 0)
    row_proj = bell_draw(streams_of[6], (E, E), E ** -0.5, 0.4375)
    w_in = bell_draw(streams_of[7], (E, HID), E ** -0.5, 0.4375)
    w_out = bell_draw(streams_of[8], (HID, E), HID ** -0.5, 0.21875)
    cotangent = bell_draw(streams_of[9], (TABLES, ROWS, FEATS, E), 1.0, 6.0, ((0, 16), (1, 16)))
    return dict(cells_in=cells_in, train_count=train_count, feat_count=feat_count, feat_qkv=feat_qkv, feat_proj=feat_proj, row_qkv=row_qkv, row_proj=row_proj, w_in=w_in, w_out=w_out, cotangent=cotangent)


def layer_norm(values):
    mean = lax.optimization_barrier(jnp.mean(values, axis=-1, keepdims=True))
    centred = values - mean
    var = lax.optimization_barrier(jnp.mean(centred * centred, axis=-1, keepdims=True))
    return centred / jnp.sqrt(var + 1e-05)

def feature_layer(block, feat_limit, weight_qkv, weight_proj):
    rows, feats, width = block.shape
    packed = jnp.dot(block.reshape(rows * feats, width), weight_qkv, preferred_element_type=jnp.float32)
    packed = packed.astype(jnp.bfloat16).reshape(rows, feats, 3, HEADS, HEAD_DIM).astype(jnp.float32)
    query, keys, values = (packed[:, :, 0], packed[:, :, 1], packed[:, :, 2])
    score = jnp.einsum('rfhd,rghd->rhfg', query, keys) / jnp.sqrt(jnp.float32(HEAD_DIM))
    keep = jnp.arange(feats, dtype=jnp.int32) < feat_limit
    score = jnp.where(keep[None, None, None, :], score, jnp.float32(-1e+30))
    probs = jax.nn.softmax(score, axis=-1).astype(jnp.bfloat16).astype(jnp.float32)
    attended = jnp.einsum('rhfg,rghd->rfhd', probs, values).astype(jnp.bfloat16)
    mixed = jnp.dot(attended.reshape(rows * feats, width), weight_proj, preferred_element_type=jnp.float32)
    total = block.reshape(rows * feats, width).astype(jnp.float32) + mixed
    return layer_norm(total).astype(jnp.bfloat16).reshape(rows, feats, width)

def row_single(column, train_limit, weight_qkv, weight_proj):
    rows, width = column.shape
    packed = jnp.dot(column, weight_qkv, preferred_element_type=jnp.float32)
    packed = packed.astype(jnp.bfloat16).reshape(rows, 3, HEADS, HEAD_DIM).astype(jnp.float32)
    query, keys, values = (packed[:, 0], packed[:, 1], packed[:, 2])
    score = jnp.einsum('ihd,jhd->hij', query, keys) / jnp.sqrt(jnp.float32(HEAD_DIM))
    keep = jnp.arange(rows, dtype=jnp.int32) < train_limit
    score = jnp.where(keep[None, None, :], score, jnp.float32(-1e+30))
    probs = jax.nn.softmax(score, axis=-1).astype(jnp.bfloat16).astype(jnp.float32)
    attended = jnp.einsum('hij,jhd->ihd', probs, values).astype(jnp.bfloat16).reshape(rows, width)
    mixed = jnp.dot(attended, weight_proj, preferred_element_type=jnp.float32)
    return layer_norm(column.astype(jnp.float32) + mixed).astype(jnp.bfloat16)

def exact_gelu(values):
    return jax.nn.gelu(values, approximate=False)

def reference(cells_in, train_count, feat_count, feat_qkv, feat_proj, row_qkv, row_proj, w_in, w_out, cotangent):

    def one_table(operands):
        block, cot_block, train_limit, feat_limit = operands
        mid = feature_layer(block, feat_limit, feat_qkv, feat_proj)
        columns = jnp.moveaxis(mid, 1, 0)
        normed_cols = lax.map(lambda column: row_single(column, train_limit, row_qkv, row_proj), columns)
        normed = jnp.moveaxis(normed_cols, 0, 1).reshape(-1, E)
        pre = jnp.dot(normed, w_in, preferred_element_type=jnp.float32)
        act_f, backward = jax.vjp(exact_gelu, pre)
        act = act_f.astype(jnp.bfloat16)
        output = (normed.astype(jnp.float32) + jnp.dot(act, w_out, preferred_element_type=jnp.float32)).astype(jnp.bfloat16)
        cot_flat = cot_block.reshape(-1, E)
        dact = jnp.dot(cot_flat, w_out.T, preferred_element_type=jnp.float32)
        dpre = backward(dact)[0].astype(jnp.bfloat16)
        part_in = jnp.dot(normed.T, dpre, preferred_element_type=jnp.float32)
        part_out = jnp.dot(act.T, cot_flat, preferred_element_type=jnp.float32)
        return (output.reshape(block.shape), part_in, part_out)
    outputs, parts_in, parts_out = lax.map(one_table, (cells_in, cotangent, train_count, feat_count))
    factor = 1.0 / jnp.sqrt(jnp.float32(TABLES * ROWS * FEATS))
    return (outputs, lax.optimization_barrier(jnp.sum(parts_in, axis=0)) * factor, lax.optimization_barrier(jnp.sum(parts_out, axis=0)) * factor)
```

```python
import functools
import math

import jax
import jax.numpy as jnp
from jax import lax
from jax.experimental import pallas as pl
from jax.experimental.pallas import tpu as pltpu
from jax.sharding import PartitionSpec as P

HEADS = 6
HEAD_DIM = 32
E = 192
HID = 768
FEATS = 112
ROWS = 512
LOCAL = 32
PEERS = 16
OWN = 7
KEYS = 384
STRIDE = 40
F32 = jnp.float32
BF16 = jnp.bfloat16
NEG = -1e30
QSCALE = math.log2(math.e) / math.sqrt(HEAD_DIM)
VMEM_LIMIT = 60 * 1024 * 1024
MESH = pl.DeviceIdType.MESH

NN = (((1,), (0,)), ((), ()))
NT = (((1,), (1,)), ((), ()))


def mm(a, b, dims=NN):
    return lax.dot_general(a, b, dims, preferred_element_type=F32)


def eye(n):
    r = lax.broadcasted_iota(jnp.int32, (n, n), 0)
    c = lax.broadcasted_iota(jnp.int32, (n, n), 1)
    return (r == c).astype(F32).astype(BF16)


def head_mask(head):
    lane = lax.broadcasted_iota(jnp.int32, (1, 128), 1)
    low = 32 * (head % 4)
    return ((lane >= low) & (lane < low + 32)).astype(F32).astype(BF16)


def ones_mask(head):
    lane = lax.broadcasted_iota(jnp.int32, (1, 128), 1)
    low = 32 * (head % 4)
    high = 128 if head == 5 else low + 32
    return ((lane >= low) & (lane < high)).astype(F32).astype(BF16)


def spread_weights(w_ref, wide_ref, proj_ref, proj_wide):
    wide_ref[...] = jnp.zeros(wide_ref.shape, BF16)
    for part in range(3):
        wide_ref[:, 256 * part : 256 * part + 192] = w_ref[:, 192 * part : 192 * part + 192]
    proj_wide[...] = jnp.zeros(proj_wide.shape, BF16)
    proj_wide[0:192, :] = proj_ref[...]


def layer_norm(total):
    mean = jnp.sum(total, axis=-1, keepdims=True) * (1.0 / E)
    centred = total - mean
    var = jnp.sum(centred * centred, axis=-1, keepdims=True) * (1.0 / E)
    return centred * lax.rsqrt(var + 1e-05)


def enter(axes):
    barrier = pltpu.get_barrier_semaphore()
    for axis in axes:
        me = lax.axis_index(axis)

        @pl.loop(1, PEERS)
        def _(k):
            pl.semaphore_signal(
                barrier, inc=1, device_id={axis: lax.rem(me + k, PEERS)}, device_id_type=MESH
            )

    pl.semaphore_wait(barrier, (PEERS - 1) * len(axes))


FBLOCK = 4


def feature_kernel(
    remote,
    count_ref,
    x_ref,
    w_ref,
    proj_ref,
    out_ref,
    wide,
    proj_wide,
    tok,
    qkv,
    vals0,
    vals1,
    att,
    turn0,
    turn1,
    send,
    send_sem,
    recv_sem,
):
    me = lax.axis_index("cells") if remote else 0
    if remote:
        enter(("cells",))
    spread_weights(w_ref, wide, proj_ref, proj_wide)
    ident = eye(FEATS)
    lane = lax.broadcasted_iota(jnp.int32, (1, 128), 1)
    bias = jnp.where(lane < count_ref[0], 0.0, NEG).astype(F32)
    for ref, heads in ((vals0, range(4)), (vals1, range(4, 6))):
        ref[...] = jnp.zeros(ref.shape, BF16)
        for j in range(FBLOCK):
            for i, h in enumerate(heads):
                ref[j, 128 * i : 128 * i + FEATS, 128:256] = jnp.broadcast_to(ones_mask(h), (FEATS, 128))
    zero_pad = jnp.zeros((128 - FEATS, 128), BF16)

    def block(step, _):
        for j in range(FBLOCK):
            tok[pl.ds(FEATS * j, FEATS), :] = mm(ident, x_ref[step * FBLOCK + j], NT)
        qkv[...] = mm(tok[...].astype(BF16), wide[...])
        for j in range(FBLOCK):
            rows = pl.ds(FEATS * j, FEATS)
            for tile, heads, vals in ((0, range(4), vals0), (1, range(4, 6), vals1)):
                at = 128 * tile
                q = (qkv[rows, at : at + 128] * QSCALE).astype(BF16)
                k = qkv[rows, 256 + at : 384 + at].astype(BF16)
                v = qkv[rows, 512 + at : 640 + at].astype(BF16)
                pieces = []
                for i, h in enumerate(heads):
                    pieces += [k * head_mask(h), zero_pad]
                    vals[j, 128 * i : 128 * i + FEATS, 0:128] = v * head_mask(h)
                score = mm(q, jnp.concatenate(pieces, axis=0), NT)
                probs = []
                for i, h in enumerate(heads):
                    s = score[:, 128 * i : 128 * i + 128] + bias
                    probs.append(jnp.exp2(s - jnp.max(s, axis=-1, keepdims=True)).astype(BF16))
                got = mm(jnp.concatenate(probs, axis=1), vals[j])
                att[rows, at : at + 128] = (got[:, :128] / got[:, 128:]).astype(BF16)
        total = tok[...] + mm(att[...], proj_wide[...])
        mid = layer_norm(total)
        for j in range(FBLOCK):
            at = step * FBLOCK + j
            turn0[pl.ds(at, FEATS, stride=STRIDE), :] = mid[FEATS * j : FEATS * j + FEATS, 0:128]
            turn1[pl.ds(at, FEATS, stride=STRIDE), 0:64] = mid[FEATS * j : FEATS * j + FEATS, 128:192]
        return 0

    def half(c, _):
        lax.fori_loop(c * (16 // FBLOCK), (c + 1) * (16 // FBLOCK), block, 0)
        base = pl.multiple_of(c * 16, 16)

        def to_peer(k, _):
            p = lax.rem(me + k, PEERS)
            for f in range(OWN):
                src = pl.multiple_of((p * OWN + f) * STRIDE + base, 8)
                send[p, f, pl.ds(base, 16), 0:128] = turn0[pl.ds(src, 16), :].astype(BF16)
                send[p, f, pl.ds(base, 16), 128:192] = turn1[pl.ds(src, 16), 0:64].astype(BF16)
            source = send.at[p, :, pl.ds(base, 16), :]
            target = out_ref.at[:, pl.ds(pl.multiple_of(me * LOCAL + base, 16), 16), :]

            if remote:

                @pl.when(k == 0)
                def _():
                    pltpu.make_async_copy(source, target, recv_sem).start()

                @pl.when(k != 0)
                def _():
                    pltpu.make_async_remote_copy(
                        src_ref=source,
                        dst_ref=target,
                        send_sem=send_sem,
                        recv_sem=recv_sem,
                        device_id={"cells": p},
                        device_id_type=MESH,
                    ).start()

            else:
                target = out_ref.at[:, pl.ds(pl.multiple_of(p * LOCAL + base, 16), 16), :]
                pltpu.make_async_copy(source, target, recv_sem).start()
            return 0

        return lax.fori_loop(0, PEERS, to_peer, 0)

    lax.fori_loop(0, 2, half, 0)
    pltpu.make_async_copy(out_ref, out_ref, recv_sem).wait()
    if remote:
        sent = send.at[pl.ds(0, PEERS - 1)]
        pltpu.make_async_copy(sent, sent, send_sem).wait()


def feature_layer(x_t, count, weight_qkv, weight_proj, remote=True):
    vmem = pl.BlockSpec(memory_space=pltpu.VMEM)
    return pl.pallas_call(
        functools.partial(feature_kernel, remote),
        name="feature_attention",
        out_shape=jax.ShapeDtypeStruct((OWN, ROWS, E), BF16),
        in_specs=[pl.BlockSpec(memory_space=pltpu.SMEM), vmem, vmem, vmem],
        out_specs=pl.BlockSpec(memory_space=pl.ANY),
        scratch_shapes=[
            pltpu.VMEM((E, 768), BF16),
            pltpu.VMEM((256, E), BF16),
            pltpu.VMEM((FBLOCK * FEATS, E), F32),
            pltpu.VMEM((FBLOCK * FEATS, 768), F32),
            pltpu.VMEM((FBLOCK, 512, 256), BF16),
            pltpu.VMEM((FBLOCK, 256, 256), BF16),
            pltpu.VMEM((FBLOCK * FEATS, 256), BF16),
            pltpu.VMEM((FEATS * STRIDE, 128), F32),
            pltpu.VMEM((FEATS * STRIDE, 128), F32),
            pltpu.VMEM((PEERS, OWN, LOCAL, E), BF16),
            pltpu.SemaphoreType.DMA,
            pltpu.SemaphoreType.DMA,
        ],
        compiler_params=pltpu.CompilerParams(
            collective_id=0 if remote else None, has_side_effects=True, vmem_limit_bytes=VMEM_LIMIT
        ),
    )(count, x_t, weight_qkv, weight_proj)


def row_kernel(
    remote,
    count_ref,
    x_ref,
    w_ref,
    proj_ref,
    out_ref,
    wide,
    proj_wide,
    qkv,
    keys,
    vals,
    att,
    done,
    send_sem,
    recv_sem,
):
    me = lax.axis_index("cells") if remote else 0
    if remote:
        enter(("cells",))
    spread_weights(w_ref, wide, proj_ref, proj_wide)
    lane = lax.broadcasted_iota(jnp.int32, (1, KEYS), 1)
    bias = jnp.where(lane < count_ref[0], 0.0, NEG).astype(F32)
    for h in range(HEADS):
        vals[KEYS * h : KEYS * h + KEYS, 128:256] = jnp.broadcast_to(ones_mask(h), (KEYS, 128))

    def column(f, _):
        x = x_ref[f]
        qkv[...] = mm(x, wide[...])
        for h in range(HEADS):
            at = 128 * (h // 4)
            rows = pl.ds(KEYS * h, KEYS)
            keys[rows, :] = qkv[0:KEYS, 256 + at : 384 + at].astype(BF16) * head_mask(h)
            vals[rows, 0:128] = qkv[0:KEYS, 512 + at : 640 + at].astype(BF16) * head_mask(h)
        for tile, pairs in ((0, (0, 2)), (1, (4,))):
            at = 128 * tile
            q = (qkv[:, at : at + 128] * QSCALE).astype(BF16)
            got = None
            for first in pairs:
                rows = pl.ds(KEYS * first, 2 * KEYS)
                score = mm(q, keys[rows, :], NT)
                probs = []
                for i in range(2):
                    s = score[:, KEYS * i : KEYS * i + KEYS] + bias
                    probs.append(jnp.exp2(s - jnp.max(s, axis=-1, keepdims=True)).astype(BF16))
                more = mm(jnp.concatenate(probs, axis=1), vals[rows, :])
                got = more if got is None else got + more
            att[:, at : at + 128] = (got[:, :128] / got[:, 128:]).astype(BF16)
        total = x.astype(F32) + mm(att[...], proj_wide[...])
        done[f] = layer_norm(total).astype(BF16)

        def to_peer(k, _):
            p = lax.rem(me + k, PEERS)
            source = done.at[f, pl.ds(pl.multiple_of(p * LOCAL, LOCAL), LOCAL), :]
            target = out_ref.at[me * OWN + f]
            if remote:

                @pl.when(k == 0)
                def _():
                    pltpu.make_async_copy(source, target, recv_sem).start()

                @pl.when(k != 0)
                def _():
                    pltpu.make_async_remote_copy(
                        src_ref=source,
                        dst_ref=target,
                        send_sem=send_sem,
                        recv_sem=recv_sem,
                        device_id={"cells": p},
                        device_id_type=MESH,
                    ).start()

            else:
                pltpu.make_async_copy(source, out_ref.at[p * OWN + f], recv_sem).start()
            return 0

        return lax.fori_loop(0, PEERS, to_peer, 0)

    lax.fori_loop(0, OWN, column, 0)
    pltpu.make_async_copy(out_ref, out_ref, recv_sem).wait()
    if remote:
        sent = out_ref.at[pl.ds(0, OWN * (PEERS - 1))]
        pltpu.make_async_copy(sent, sent, send_sem).wait()


def row_layer(columns, count, weight_qkv, weight_proj, remote=True):
    vmem = pl.BlockSpec(memory_space=pltpu.VMEM)
    return pl.pallas_call(
        functools.partial(row_kernel, remote),
        name="row_attention",
        out_shape=jax.ShapeDtypeStruct((FEATS, LOCAL, E), BF16),
        in_specs=[pl.BlockSpec(memory_space=pltpu.SMEM), vmem, vmem, vmem],
        out_specs=pl.BlockSpec(memory_space=pl.ANY),
        scratch_shapes=[
            pltpu.VMEM((E, 768), BF16),
            pltpu.VMEM((256, E), BF16),
            pltpu.VMEM((ROWS, 768), F32),
            pltpu.VMEM((HEADS * KEYS, 128), BF16),
            pltpu.VMEM((HEADS * KEYS, 256), BF16),
            pltpu.VMEM((ROWS, 256), BF16),
            pltpu.VMEM((OWN, ROWS, E), BF16),
            pltpu.SemaphoreType.DMA,
            pltpu.SemaphoreType.DMA,
        ],
        compiler_params=pltpu.CompilerParams(
            collective_id=1 if remote else None, has_side_effects=True, vmem_limit_bytes=VMEM_LIMIT
        ),
    )(count, columns, weight_qkv, weight_proj)


DROWS = 4
DTOK = DROWS * 128
HBLOCK = 256


def dense_kernel(
    x_ref, cot_ref, win_ref, wout_ref, out_ref, grad_ref, turn0, turn1, win_t, wout, wout_t, tok, cot, sums
):
    new = lax.broadcasted_iota(jnp.int32, (HID, HID), 0)
    old = lax.broadcasted_iota(jnp.int32, (HID, HID), 1)
    cell = new // 48
    table = (new - cell * 48) // 3
    place = table * 48 + cell * 3 + (new - cell * 48 - table * 3)
    perm = (old == place).astype(F32).astype(BF16)
    win_t[...] = mm(perm, win_ref[...], NT).astype(BF16)
    wout[...] = mm(perm, wout_ref[...], NT).astype(BF16)
    wout_t[...] = mm(wout_ref[...], perm, NT).astype(BF16)
    sums[...] = jnp.zeros(sums.shape, F32)
    tok[...] = jnp.zeros(tok.shape, BF16)
    cot[...] = jnp.zeros(cot.shape, BF16)
    ident = eye(E)

    def unpack(f, _):
        at = pl.multiple_of(f * STRIDE, 8)
        turn0[pl.ds(at, LOCAL), :] = x_ref[f, :, 0:128].astype(F32)
        turn1[pl.ds(at, LOCAL), 0:64] = x_ref[f, :, 128:192].astype(F32)
        return 0

    lax.fori_loop(0, FEATS, unpack, 0, unroll=4)

    def block(step, _):
        for j in range(DROWS):
            at = step * DROWS + j
            tok[128 * j : 128 * j + FEATS, 0:128] = turn0[pl.ds(at, FEATS, stride=STRIDE), :].astype(BF16)
            tok[128 * j : 128 * j + FEATS, 128:192] = turn1[pl.ds(at, FEATS, stride=STRIDE), 0:64].astype(BF16)
            cot[:, 128 * j : 128 * j + FEATS] = cot_ref[at]
        x = tok[...]
        c = cot[...]
        total = mm(ident, x, NT)
        for hb in range(HID // HBLOCK):
            rows = pl.ds(HBLOCK * hb, HBLOCK)
            pre = mm(win_t[rows, :], x, NT)
            cdf = 0.5 * lax.erf(pre * math.sqrt(0.5)) + 0.5
            act = (pre * cdf).astype(BF16)
            slope = cdf + pre * (jnp.exp2(pre * pre * (-0.5 * math.log2(math.e))) * (1.0 / math.sqrt(2 * math.pi)))
            dpre = (mm(wout[rows, :], c) * slope).astype(BF16)
            sums[0, rows, :] += mm(dpre, x)
            sums[1, rows, :] += mm(act, c, NT)
            total = total + mm(wout_t[:, HBLOCK * hb : HBLOCK * hb + HBLOCK], act)
        for j in range(DROWS):
            out_ref[step * DROWS + j] = total[:, 128 * j : 128 * j + FEATS].astype(BF16)
        return 0

    lax.fori_loop(0, LOCAL // DROWS, block, 0)
    factor = 1.0 / math.sqrt(16 * ROWS * FEATS)
    grad_ref[...] = (sums[...] * factor).astype(BF16)


def dense_layer(x, cot_t, w_in, w_out_t):
    vmem = pl.BlockSpec(memory_space=pltpu.VMEM)
    return pl.pallas_call(
        dense_kernel,
        name="feed_forward",
        out_shape=(
            jax.ShapeDtypeStruct((LOCAL, E, FEATS), BF16),
            jax.ShapeDtypeStruct((2, HID, E), BF16),
        ),
        in_specs=[vmem] * 4,
        out_specs=(vmem, vmem),
        scratch_shapes=[
            pltpu.VMEM((FEATS * STRIDE, 128), F32),
            pltpu.VMEM((FEATS * STRIDE, 128), F32),
            pltpu.VMEM((HID, E), BF16),
            pltpu.VMEM((HID, E), BF16),
            pltpu.VMEM((E, HID), BF16),
            pltpu.VMEM((DTOK, E), BF16),
            pltpu.VMEM((E, DTOK), BF16),
            pltpu.VMEM((2, HID, E), F32),
        ],
        compiler_params=pltpu.CompilerParams(vmem_limit_bytes=VMEM_LIMIT),
    )(x, cot_t, w_in, w_out_t)


def sums_kernel(part_ref, in_ref, out_ref, got, mid, got2, send_sem, recv_sem, send_sem2, recv_sem2):
    cell = lax.axis_index("cells")
    table = lax.axis_index("tables")
    enter(("cells", "tables"))

    def exchange(axis, me, source_of, landing, send_s, recv_s):
        @pl.loop(0, PEERS)
        def _(k):
            p = lax.rem(me + k, PEERS)

            @pl.when(k == 0)
            def _():
                pltpu.make_async_copy(source_of(p), landing.at[me], recv_s).start()

            @pl.when(k != 0)
            def _():
                pltpu.make_async_remote_copy(
                    src_ref=source_of(p),
                    dst_ref=landing.at[me],
                    send_sem=send_s,
                    recv_sem=recv_s,
                    device_id={axis: p},
                    device_id_type=MESH,
                ).start()

        pltpu.make_async_copy(landing, landing, recv_s).wait()
        sent = landing.at[pl.ds(0, PEERS - 1)]
        pltpu.make_async_copy(sent, sent, send_s).wait()

    exchange(
        "cells",
        cell,
        lambda p: part_ref.at[:, pl.ds(pl.multiple_of(48 * p, 16), 48), :],
        got,
        send_sem,
        recv_sem,
    )
    total = got[0].astype(F32)
    for p in range(1, PEERS):
        total = total + got[p].astype(F32)
    mid[...] = jnp.zeros(mid.shape, F32)
    for t in range(PEERS):
        mid[t, 0:3, :] = total[0, 3 * t : 3 * t + 3, :]
        mid[t, 4:7, :] = total[1, 3 * t : 3 * t + 3, :]
    exchange("tables", table, lambda p: mid.at[p], got2, send_sem2, recv_sem2)
    final = got2[0]
    for t in range(1, PEERS):
        final = final + got2[t]
    in_ref[...] = final[0:3, :]
    out_ref[...] = final[4:7, :]


def sum_grads(part):
    vmem = pl.BlockSpec(memory_space=pltpu.VMEM)
    return pl.pallas_call(
        sums_kernel,
        name="weight_gradient_sums",
        out_shape=(jax.ShapeDtypeStruct((3, E), F32), jax.ShapeDtypeStruct((3, E), F32)),
        in_specs=[vmem],
        out_specs=(vmem, vmem),
        scratch_shapes=[
            pltpu.VMEM((PEERS, 2, 48, E), BF16),
            pltpu.VMEM((PEERS, 8, E), F32),
            pltpu.VMEM((PEERS, 8, E), F32),
            pltpu.SemaphoreType.DMA,
            pltpu.SemaphoreType.DMA,
            pltpu.SemaphoreType.DMA,
            pltpu.SemaphoreType.DMA,
        ],
        compiler_params=pltpu.CompilerParams(
            collective_id=2, has_side_effects=True, vmem_limit_bytes=VMEM_LIMIT
        ),
    )(part)


def per_device(
    cells_in, train_count, feat_count, feat_qkv, feat_proj, row_qkv, row_proj, w_in, w_out, cotangent
):
    x_t = jnp.swapaxes(cells_in[0], 1, 2)
    cot_t = jnp.swapaxes(cotangent[0], 1, 2)
    columns = feature_layer(x_t, feat_count, feat_qkv, feat_proj)
    normed = row_layer(columns, train_count, row_qkv, row_proj)
    out_t, part = dense_layer(normed, cot_t, w_in, w_out.T)
    grad_in, grad_out = sum_grads(part)
    return (jnp.swapaxes(out_t, 1, 2)[None], grad_in.T, grad_out)


def solution(mesh):
    return jax.shard_map(
        per_device,
        mesh=mesh,
        in_specs=(
            P("tables", "cells", None, None),
            P("tables"),
            P("tables"),
            P(),
            P(),
            P(),
            P(),
            P(),
            P(),
            P("tables", "cells", None, None),
        ),
        out_specs=(
            P("tables", "cells", None, None),
            P(None, ("tables", "cells")),
            P(("tables", "cells"), None),
        ),
        check_vma=False,
    )
```

```python
import functools
import math

import jax
import jax.numpy as jnp
from jax import lax
from jax.experimental import pallas as pl
from jax.experimental.pallas import tpu as pltpu
from jax.sharding import PartitionSpec as P

HEADS = 6
HEAD_DIM = 32
E = 192
HID = 768
FEATS = 112
ROWS = 512
LOCAL = 32
PEERS = 16
OWN = 7
KEYS = 384
STRIDE = 40
F32 = jnp.float32
BF16 = jnp.bfloat16
NEG = -1e30
QSCALE = math.log2(math.e) / math.sqrt(HEAD_DIM)
ATTENTION_VMEM = 60 * 1024 * 1024
DENSE_VMEM = 60 * 1024 * 1024
SUMS_VMEM = 8 * 1024 * 1024
MESH = pl.DeviceIdType.MESH

NN = (((1,), (0,)), ((), ()))
NT = (((1,), (1,)), ((), ()))


def mm(a, b, dims=NN):
    return lax.dot_general(a, b, dims, preferred_element_type=F32)


def eye(n):
    r = lax.broadcasted_iota(jnp.int32, (n, n), 0)
    c = lax.broadcasted_iota(jnp.int32, (n, n), 1)
    return (r == c).astype(F32).astype(BF16)


def head_mask(head):
    lane = lax.broadcasted_iota(jnp.int32, (1, 128), 1)
    low = 32 * (head % 4)
    return ((lane >= low) & (lane < low + 32)).astype(F32).astype(BF16)


def ones_mask(head):
    lane = lax.broadcasted_iota(jnp.int32, (1, 128), 1)
    low = 32 * (head % 4)
    high = 128 if head == 5 else low + 32
    return ((lane >= low) & (lane < high)).astype(F32).astype(BF16)


def spread_weights(w_ref, wide_ref, proj_ref, proj_wide):
    wide_ref[...] = jnp.zeros(wide_ref.shape, BF16)
    for part in range(3):
        wide_ref[0:192, 256 * part : 256 * part + 192] = w_ref[:, 192 * part : 192 * part + 192]
    proj_wide[...] = jnp.zeros(proj_wide.shape, BF16)
    proj_wide[0:192, 0:192] = proj_ref[...]


def layer_norm(low, high):
    mean = (jnp.sum(low, axis=-1, keepdims=True) + jnp.sum(high, axis=-1, keepdims=True)) * (1.0 / E)
    low = low - mean
    half = lax.broadcasted_iota(jnp.int32, (1, 128), 1) < 64
    high = jnp.where(half, high - mean, 0.0)
    var = jnp.sum(low * low + high * high, axis=-1, keepdims=True) * (1.0 / E)
    scale = lax.rsqrt(var + 1e-05)
    return low * scale, high * scale


def greet(axes):
    barrier = pltpu.get_barrier_semaphore()
    for axis in axes:
        me = lax.axis_index(axis)

        @pl.loop(1, PEERS)
        def _(k):
            pl.semaphore_signal(
                barrier, inc=1, device_id={axis: lax.rem(me + k, PEERS)}, device_id_type=MESH
            )


def await_peers(axes):
    pl.semaphore_wait(pltpu.get_barrier_semaphore(), (PEERS - 1) * len(axes))


FBLOCK = 4
TILES = 11


def attention_kernel(
    remote,
    feat_count,
    train_count,
    x_ref,
    fw_ref,
    fproj_ref,
    rw_ref,
    rproj_ref,
    out_ref,
    fwide,
    fproj,
    rwide,
    rproj,
    tok,
    qkv,
    vals0,
    vals1,
    att,
    turn0,
    turn1,
    send,
    cols,
    rq,
    rkv,
    keys,
    vals,
    ratt,
    done,
    send_sem,
    cols_sem,
    send2_sem,
    recv2_sem,
):
    me = lax.axis_index("cells") if remote else 0
    if remote:
        greet(("cells",))
    spread_weights(fw_ref, fwide, fproj_ref, fproj)
    ident = eye(FEATS)
    tok[:, 192:256] = jnp.zeros((FBLOCK * FEATS, 64), F32)
    lane = lax.broadcasted_iota(jnp.int32, (1, 128), 1)
    bias = jnp.where(lane < feat_count[0], 0.0, NEG).astype(F32)
    for ref, heads in ((vals0, range(4)), (vals1, range(4, 6))):
        ref[...] = jnp.zeros(ref.shape, BF16)
        for j in range(FBLOCK):
            for i, h in enumerate(heads):
                ref[j, 128 * i : 128 * i + FEATS, 128:256] = jnp.broadcast_to(ones_mask(h), (FEATS, 128))
    zero_pad = jnp.zeros((128 - FEATS, 128), BF16)

    def block(step, _):
        for j in range(FBLOCK):
            tok[pl.ds(FEATS * j, FEATS), 0:192] = mm(ident, x_ref[step * FBLOCK + j], NT)
        qkv[...] = mm(tok[...].astype(BF16), fwide[...])
        for j in range(FBLOCK):
            rows = pl.ds(FEATS * j, FEATS)
            for tile, heads, ref in ((0, range(4), vals0), (1, range(4, 6), vals1)):
                at = 128 * tile
                q = (qkv[rows, at : at + 128] * QSCALE).astype(BF16)
                k = qkv[rows, 256 + at : 384 + at].astype(BF16)
                v = qkv[rows, 512 + at : 640 + at].astype(BF16)
                pieces = []
                for i, h in enumerate(heads):
                    pieces += [k * head_mask(h), zero_pad]
                    ref[j, 128 * i : 128 * i + FEATS, 0:128] = v * head_mask(h)
                score = mm(q, jnp.concatenate(pieces, axis=0), NT)
                probs = []
                for i, h in enumerate(heads):
                    s = score[:, 128 * i : 128 * i + 128] + bias
                    probs.append(jnp.exp2(s - jnp.max(s, axis=-1, keepdims=True)).astype(BF16))
                got = mm(jnp.concatenate(probs, axis=1), ref[j])
                att[rows, at : at + 128] = (got[:, :128] / got[:, 128:]).astype(BF16)
        mixed = mm(att[...], fproj[...])
        low, high = layer_norm(tok[:, 0:128] + mixed[:, 0:128], tok[:, 128:256] + mixed[:, 128:256])
        for j in range(FBLOCK):
            at = step * FBLOCK + j
            turn0[pl.ds(at, FEATS, stride=STRIDE), :] = low[FEATS * j : FEATS * j + FEATS]
            turn1[pl.ds(at, FEATS, stride=STRIDE), :] = high[FEATS * j : FEATS * j + FEATS]
        return 0

    def pack(p, group, base):
        def rows_of(ref, f):
            return ref[pl.ds(pl.multiple_of((p * OWN + f) * STRIDE + base, 8), 16), :]

        f = 2 * group
        at = 3 * group
        send[p, at, pl.ds(base, 16), :] = rows_of(turn0, f).astype(BF16)
        high = rows_of(turn1, f)
        if f + 1 < OWN:
            at += 1
            send[p, at, pl.ds(base, 16), :] = rows_of(turn0, f + 1).astype(BF16)
            high = high + pltpu.roll(rows_of(turn1, f + 1), 64, 1)
        send[p, at + 1, pl.ds(base, 16), :] = high.astype(BF16)

    def pass_on(source, target, k, axis, p, send_s, recv_s):
        if not remote:
            pltpu.make_async_copy(source, target, recv_s).start()
            return

        @pl.when(k == 0)
        def _():
            pltpu.make_async_copy(source, target, recv_s).start()

        @pl.when(k != 0)
        def _():
            pltpu.make_async_remote_copy(
                src_ref=source,
                dst_ref=target,
                send_sem=send_s,
                recv_sem=recv_s,
                device_id={axis: p},
                device_id_type=MESH,
            ).start()

    def place(p):
        return pl.multiple_of((me if remote else p) * LOCAL, LOCAL)

    lax.fori_loop(0, 16 // FBLOCK, block, 0)
    if remote:
        await_peers(("cells",))

    def first_half(k, _):
        p = lax.rem(me + k, PEERS)
        for group in range(4):
            pack(p, group, 0)
        pass_on(
            send.at[p, :, pl.ds(0, 16), :],
            cols.at[:, pl.ds(place(p), 16), :],
            k,
            "cells",
            p,
            send_sem,
            cols_sem.at[4],
        )
        return 0

    lax.fori_loop(0, PEERS, first_half, 0)
    lax.fori_loop(16 // FBLOCK, 32 // FBLOCK, block, 0)
    for group in range(4):
        tiles = pl.ds(3 * group, min(3, TILES - 3 * group))

        def second_half(k, _):
            p = lax.rem(me + k, PEERS)
            pack(p, group, 16)
            pass_on(
                send.at[p, tiles, pl.ds(16, 16), :],
                cols.at[tiles, pl.ds(place(p) + 16, 16), :],
                k,
                "cells",
                p,
                send_sem,
                cols_sem.at[group],
            )
            return 0

        lax.fori_loop(0, PEERS, second_half, 0)

    spread_weights(rw_ref, rwide, rproj_ref, rproj)
    lane = lax.broadcasted_iota(jnp.int32, (1, KEYS), 1)
    rbias = jnp.where(lane < train_count[0], 0.0, NEG).astype(F32)
    for h in range(HEADS):
        vals[KEYS * h : KEYS * h + KEYS, 128:256] = jnp.broadcast_to(ones_mask(h), (KEYS, 128))
    half_lane = lax.broadcasted_iota(jnp.int32, (1, 128), 1) < 64

    def column(f, _):
        @pl.when(f == 0)
        def _():
            ref = cols.at[:, pl.ds(0, ROWS // 2), :]
            pltpu.make_async_copy(ref, ref, cols_sem.at[4]).wait()

        for group in range(4):

            @pl.when(f == 2 * group)
            def _():
                ref = cols.at[pl.ds(3 * group, min(3, TILES - 3 * group)), pl.ds(0, ROWS // 2), :]
                pltpu.make_async_copy(ref, ref, cols_sem.at[group]).wait()

        odd = lax.rem(f, 2)
        at = 3 * (f // 2)
        low = cols[at + odd]
        high = cols[jnp.minimum(at + 2, TILES - 1)].astype(F32)
        high = jnp.where(half_lane, pltpu.roll(high, 64 * odd, 1), 0.0)
        x = jnp.concatenate([low, high.astype(BF16)], axis=1)
        rq[...] = (mm(x, rwide[:, 0:256]) * QSCALE).astype(BF16)
        rkv[...] = mm(x[0:KEYS], rwide[:, 256:768]).astype(BF16)
        for h in range(HEADS):
            at = 128 * (h // 4)
            rows = pl.ds(KEYS * h, KEYS)
            keys[rows, :] = rkv[:, at : at + 128] * head_mask(h)
            vals[rows, 0:128] = rkv[:, 256 + at : 384 + at] * head_mask(h)
        for tile, pairs in ((0, (0, 2)), (1, (4,))):
            at = 128 * tile
            got = None
            for first in pairs:
                rows = pl.ds(KEYS * first, 2 * KEYS)
                score = mm(rq[:, at : at + 128], keys[rows, :], NT)
                probs = []
                for i in range(2):
                    s = score[:, KEYS * i : KEYS * i + KEYS] + rbias
                    probs.append(jnp.exp2(s - jnp.max(s, axis=-1, keepdims=True)).astype(BF16))
                more = mm(jnp.concatenate(probs, axis=1), vals[rows, :])
                got = more if got is None else got + more
            ratt[:, at : at + 128] = (got[:, :128] / got[:, 128:]).astype(BF16)
        mixed = mm(ratt[...], rproj[...])
        low, high = layer_norm(low.astype(F32) + mixed[:, 0:128], high + mixed[:, 128:256])
        done[f, :, 0:32, :] = low.astype(BF16).reshape(PEERS, 32, 128)
        high = high.reshape(PEERS, 2, 16, 128)
        high = high[:, 0] + pltpu.roll(high[:, 1].reshape(PEERS * 16, 128), 64, 1).reshape(PEERS, 16, 128)
        done[f, :, 32:48, :] = high.astype(BF16)

        def to_peer(k, _):
            p = lax.rem(me + k, PEERS)
            pass_on(
                done.at[f, p],
                out_ref.at[(me if remote else p) * OWN + f],
                k,
                "cells",
                p,
                send2_sem,
                recv2_sem,
            )
            return 0

        return lax.fori_loop(0, PEERS, to_peer, 0)

    lax.fori_loop(0, OWN, column, 0)
    if remote:
        sent = send.at[pl.ds(0, PEERS - 1)]
        pltpu.make_async_copy(sent, sent, send_sem).wait()
        sent = out_ref.at[pl.ds(0, OWN * (PEERS - 1))]
        pltpu.make_async_copy(sent, sent, send2_sem).wait()
    pltpu.make_async_copy(out_ref, out_ref, recv2_sem).wait()


def attention_layers(x_t, feat_count, train_count, feat_qkv, feat_proj, row_qkv, row_proj, remote=True):
    vmem = pl.BlockSpec(memory_space=pltpu.VMEM)
    smem = pl.BlockSpec(memory_space=pltpu.SMEM)
    return pl.pallas_call(
        functools.partial(attention_kernel, remote),
        name="attention",
        out_shape=jax.ShapeDtypeStruct((FEATS, 48, 128), BF16),
        in_specs=[smem, smem] + [vmem] * 5,
        out_specs=pl.BlockSpec(memory_space=pl.ANY),
        scratch_shapes=[
            pltpu.VMEM((256, 768), BF16),
            pltpu.VMEM((256, 256), BF16),
            pltpu.VMEM((256, 768), BF16),
            pltpu.VMEM((256, 256), BF16),
            pltpu.VMEM((FBLOCK * FEATS, 256), F32),
            pltpu.VMEM((FBLOCK * FEATS, 768), F32),
            pltpu.VMEM((FBLOCK, 512, 256), BF16),
            pltpu.VMEM((FBLOCK, 256, 256), BF16),
            pltpu.VMEM((FBLOCK * FEATS, 256), BF16),
            pltpu.VMEM((FEATS * STRIDE, 128), F32),
            pltpu.VMEM((FEATS * STRIDE, 128), F32),
            pltpu.VMEM((PEERS, TILES, LOCAL, 128), BF16),
            pltpu.VMEM((TILES, ROWS, 128), BF16),
            pltpu.VMEM((ROWS, 256), BF16),
            pltpu.VMEM((KEYS, 512), BF16),
            pltpu.VMEM((HEADS * KEYS, 128), BF16),
            pltpu.VMEM((HEADS * KEYS, 256), BF16),
            pltpu.VMEM((ROWS, 256), BF16),
            pltpu.VMEM((OWN, PEERS, 48, 128), BF16),
            pltpu.SemaphoreType.DMA,
            pltpu.SemaphoreType.DMA((5,)),
            pltpu.SemaphoreType.DMA,
            pltpu.SemaphoreType.DMA,
        ],
        compiler_params=pltpu.CompilerParams(
            collective_id=0 if remote else None, has_side_effects=True, vmem_limit_bytes=ATTENTION_VMEM
        ),
    )(feat_count, train_count, x_t, feat_qkv, feat_proj, row_qkv, row_proj)


DROWS = 4
DTOK = DROWS * 128
HBLOCK = 256


def dense_kernel(
    x_ref, cot_ref, win_ref, wout_ref, out_ref, grad_ref, turn0, turn1, win_t, wout, wout_t, tok, cot, sums
):
    new = lax.broadcasted_iota(jnp.int32, (HID, 1), 0)
    old = lax.broadcasted_iota(jnp.int32, (HID, HID), 1)
    core = new // 384
    chip = (new - core * 384) // 48
    within = new - core * 384 - chip * 48
    table = within // 3
    place = table * 48 + (2 * chip + core) * 3 + (within - table * 3)
    perm = (old == place).astype(F32).astype(BF16)
    win_t[...] = mm(perm, win_ref[...], NT).astype(BF16)
    wout[...] = (0.5 * mm(perm, wout_ref[...], NT)).astype(BF16)
    wout_t[...] = (0.5 * mm(wout_ref[...], perm, NT)).astype(BF16)
    sums[...] = jnp.zeros(sums.shape, F32)
    tok[...] = jnp.zeros(tok.shape, BF16)
    cot[...] = jnp.zeros(cot.shape, BF16)
    ident = eye(E)

    def unpack(f, _):
        at = pl.multiple_of(f * STRIDE, 8)
        turn0[pl.ds(at, LOCAL), :] = x_ref[f, 0:32, :].astype(F32)
        high = x_ref[f, 32:48, :].astype(F32)
        turn1[pl.ds(at, 16), :] = high
        turn1[pl.ds(at + 16, 16), :] = pltpu.roll(high, 64, 1)
        return 0

    lax.fori_loop(0, FEATS, unpack, 0, unroll=4)

    def block(step, _):
        for j in range(DROWS):
            at = step * DROWS + j
            tok[128 * j : 128 * j + FEATS, 0:128] = turn0[pl.ds(at, FEATS, stride=STRIDE), :].astype(BF16)
            tok[128 * j : 128 * j + FEATS, 128:192] = turn1[pl.ds(at, FEATS, stride=STRIDE), 0:64].astype(BF16)
            cot[:, 128 * j : 128 * j + FEATS] = cot_ref[at]
        x = tok[...]
        c = cot[...]
        total = mm(ident, x, NT)
        for hb in range(HID // HBLOCK):
            rows = pl.ds(HBLOCK * hb, HBLOCK)
            pre = mm(win_t[rows, :], x, NT)
            u = pre * math.sqrt(0.5)
            twice = lax.erf(u) + 1.0
            act = (pre * twice).astype(BF16)
            slope = twice + u * jnp.exp2(math.log2(2.0 / math.sqrt(math.pi)) - (u * u) * math.log2(math.e))
            dpre = (mm(wout[rows, :], c) * slope).astype(BF16)
            sums[0, rows, :] += mm(dpre, x)
            sums[1, rows, :] += mm(act, c, NT)
            total = total + mm(wout_t[:, HBLOCK * hb : HBLOCK * hb + HBLOCK], act)
        for j in range(DROWS):
            out_ref[step * DROWS + j] = total[:, 128 * j : 128 * j + FEATS].astype(BF16)
        return 0

    lax.fori_loop(0, LOCAL // DROWS, block, 0)
    factor = 1.0 / math.sqrt(16 * ROWS * FEATS)
    grad_ref[0] = (sums[0, :, 0:128] * factor).astype(BF16)
    grad_ref[1] = (sums[1, :, 0:128] * (0.5 * factor)).astype(BF16)
    grad_ref[2, :, 0:64] = (sums[0, :, 128:192] * factor).astype(BF16)
    grad_ref[2, :, 64:128] = (sums[1, :, 128:192] * (0.5 * factor)).astype(BF16)


def dense_layer(x, cot_t, w_in, w_out_t):
    vmem = pl.BlockSpec(memory_space=pltpu.VMEM)
    return pl.pallas_call(
        dense_kernel,
        name="feed_forward",
        out_shape=(
            jax.ShapeDtypeStruct((LOCAL, E, FEATS), BF16),
            jax.ShapeDtypeStruct((3, HID, 128), BF16),
        ),
        in_specs=[vmem] * 4,
        out_specs=(vmem, vmem),
        scratch_shapes=[
            pltpu.VMEM((FEATS * STRIDE, 128), F32),
            pltpu.VMEM((FEATS * STRIDE, 128), F32),
            pltpu.VMEM((HID, E), BF16),
            pltpu.VMEM((HID, E), BF16),
            pltpu.VMEM((E, HID), BF16),
            pltpu.VMEM((DTOK, E), BF16),
            pltpu.VMEM((E, DTOK), BF16),
            pltpu.VMEM((2, HID, E), F32),
        ],
        compiler_params=pltpu.CompilerParams(vmem_limit_bytes=DENSE_VMEM),
    )(x, cot_t, w_in, w_out_t)


CHIPS = PEERS // 2


def sums_kernel(part_ref, in_ref, out_ref, pair, half, got, mid, row, got2, sems):
    cell = lax.axis_index("cells")
    table = lax.axis_index("tables")
    chip = cell // 2
    core = cell - 2 * chip
    greet(("cells", "tables"))
    await_peers(("cells", "tables"))

    theirs = pl.ds(pl.multiple_of((1 - core) * 384, 384), 384)
    mine = pl.ds(pl.multiple_of(core * 384, 384), 384)
    swap = pltpu.make_async_remote_copy(
        src_ref=part_ref.at[:, theirs, :],
        dst_ref=pair,
        send_sem=sems.at[0],
        recv_sem=sems.at[1],
        device_id={"cells": 2 * chip + 1 - core},
        device_id_type=MESH,
    )
    swap.start()
    swap.wait()
    for t in range(3):
        half[t] = (part_ref[t, mine, :].astype(F32) + pair[t].astype(F32)).astype(BF16)

    def exchange(count, me, axis, place_of, source_of, landing, send_s, recv_s):
        @pl.loop(0, count)
        def _(k):
            p = lax.rem(me + k, count)

            @pl.when(k == 0)
            def _():
                pltpu.make_async_copy(source_of(p), landing.at[me], recv_s).start()

            @pl.when(k != 0)
            def _():
                pltpu.make_async_remote_copy(
                    src_ref=source_of(p),
                    dst_ref=landing.at[me],
                    send_sem=send_s,
                    recv_sem=recv_s,
                    device_id={axis: place_of(p)},
                    device_id_type=MESH,
                ).start()

        pltpu.make_async_copy(landing, landing, recv_s).wait()

    exchange(
        CHIPS,
        chip,
        "cells",
        lambda p: 2 * p + core,
        lambda p: half.at[:, pl.ds(pl.multiple_of(48 * p, 16), 48), :],
        got,
        sems.at[2],
        sems.at[3],
    )
    total = got[0].astype(F32)
    for p in range(1, CHIPS):
        total = total + got[p].astype(F32)
    mid[...] = jnp.zeros(mid.shape, F32)
    for t in range(PEERS):
        for i in range(3):
            mid[t, 4 * i : 4 * i + 3, :] = total[i, 3 * t : 3 * t + 3, :]
    row[...] = mid[...].astype(BF16)
    exchange(PEERS, table, "tables", lambda p: p, lambda p: row.at[p], got2, sems.at[4], sems.at[5])
    final = got2[0].astype(F32)
    for t in range(1, PEERS):
        final = final + got2[t].astype(F32)
    in_ref[:, 0:128] = final[0:3, :]
    in_ref[:, 128:192] = final[8:11, 0:64]
    out_ref[:, 0:128] = final[4:7, :]
    out_ref[:, 128:192] = final[8:11, 64:128]
    sent = got.at[pl.ds(0, CHIPS - 1)]
    pltpu.make_async_copy(sent, sent, sems.at[2]).wait()
    sent = got2.at[pl.ds(0, PEERS - 1)]
    pltpu.make_async_copy(sent, sent, sems.at[4]).wait()


def sum_grads(part):
    vmem = pl.BlockSpec(memory_space=pltpu.VMEM)
    return pl.pallas_call(
        sums_kernel,
        name="weight_gradient_sums",
        out_shape=(jax.ShapeDtypeStruct((3, E), F32), jax.ShapeDtypeStruct((3, E), F32)),
        in_specs=[vmem],
        out_specs=(vmem, vmem),
        scratch_shapes=[
            pltpu.VMEM((3, 384, 128), BF16),
            pltpu.VMEM((3, 384, 128), BF16),
            pltpu.VMEM((CHIPS, 3, 48, 128), BF16),
            pltpu.VMEM((PEERS, 16, 128), F32),
            pltpu.VMEM((PEERS, 16, 128), BF16),
            pltpu.VMEM((PEERS, 16, 128), BF16),
            pltpu.SemaphoreType.DMA((6,)),
        ],
        compiler_params=pltpu.CompilerParams(
            collective_id=2, has_side_effects=True, vmem_limit_bytes=SUMS_VMEM
        ),
    )(part)


def per_device(
    cells_in, train_count, feat_count, feat_qkv, feat_proj, row_qkv, row_proj, w_in, w_out, cotangent
):
    x_t = jnp.swapaxes(cells_in[0], 1, 2)
    cot_t = jnp.swapaxes(cotangent[0], 1, 2)
    normed = attention_layers(x_t, feat_count, train_count, feat_qkv, feat_proj, row_qkv, row_proj)
    out_t, part = dense_layer(normed, cot_t, w_in, w_out.T)
    grad_in, grad_out = sum_grads(part)
    return (jnp.swapaxes(out_t, 1, 2)[None], grad_in.T, grad_out)


def solution(mesh):
    return jax.shard_map(
        per_device,
        mesh=mesh,
        in_specs=(
            P("tables", "cells", None, None),
            P("tables"),
            P("tables"),
            P(),
            P(),
            P(),
            P(),
            P(),
            P(),
            P("tables", "cells", None, None),
        ),
        out_specs=(
            P("tables", "cells", None, None),
            P(None, ("tables", "cells")),
            P(("tables", "cells"), None),
        ),
        check_vma=False,
    )
```

```python
import functools
import math

import jax
import jax.numpy as jnp
from jax import lax
from jax.experimental import pallas as pl
from jax.experimental.pallas import tpu as pltpu
from jax.sharding import PartitionSpec as P

HEADS = 6
HEAD_DIM = 32
E = 192
HID = 768
FEATS = 112
ROWS = 512
LOCAL = 32
PEERS = 16
OWN = 7
KEYS = 384
STRIDE = 40
F32 = jnp.float32
BF16 = jnp.bfloat16
NEG = -1e30
QSCALE = math.log2(math.e) / math.sqrt(HEAD_DIM)
VMEM_LIMIT = 60 * 1024 * 1024
MESH = pl.DeviceIdType.MESH

NN = (((1,), (0,)), ((), ()))
NT = (((1,), (1,)), ((), ()))


def mm(a, b, dims=NN):
    return lax.dot_general(a, b, dims, preferred_element_type=F32)


def eye(n):
    r = lax.broadcasted_iota(jnp.int32, (n, n), 0)
    c = lax.broadcasted_iota(jnp.int32, (n, n), 1)
    return (r == c).astype(F32).astype(BF16)


def head_mask(head):
    lane = lax.broadcasted_iota(jnp.int32, (1, 128), 1)
    low = 32 * (head % 4)
    return ((lane >= low) & (lane < low + 32)).astype(F32).astype(BF16)


def ones_mask(head):
    lane = lax.broadcasted_iota(jnp.int32, (1, 128), 1)
    low = 32 * (head % 4)
    high = 128 if head == 5 else low + 32
    return ((lane >= low) & (lane < high)).astype(F32).astype(BF16)


def spread_weights(w_ref, wide_ref, proj_ref, proj_wide):
    wide_ref[...] = jnp.zeros(wide_ref.shape, BF16)
    for part in range(3):
        wide_ref[0:192, 256 * part : 256 * part + 192] = w_ref[:, 192 * part : 192 * part + 192]
    proj_wide[...] = jnp.zeros(proj_wide.shape, BF16)
    proj_wide[0:192, 0:192] = proj_ref[...]


def layer_norm(low, high):
    mean = (jnp.sum(low, axis=-1, keepdims=True) + jnp.sum(high, axis=-1, keepdims=True)) * (1.0 / E)
    low = low - mean
    half = lax.broadcasted_iota(jnp.int32, (1, 128), 1) < 64
    high = jnp.where(half, high - mean, 0.0)
    var = jnp.sum(low * low + high * high, axis=-1, keepdims=True) * (1.0 / E)
    scale = lax.rsqrt(var + 1e-05)
    return low * scale, high * scale


def greet(axes):
    barrier = pltpu.get_barrier_semaphore()
    for axis in axes:
        me = lax.axis_index(axis)

        @pl.loop(1, PEERS)
        def _(k):
            pl.semaphore_signal(
                barrier, inc=1, device_id={axis: lax.rem(me + k, PEERS)}, device_id_type=MESH
            )


def await_peers(axes):
    pl.semaphore_wait(pltpu.get_barrier_semaphore(), (PEERS - 1) * len(axes))


DROWS = 4
DTOK = DROWS * 128
HBLOCK = 256
CHIPS = PEERS // 2


def order_hidden(win_ref, wout_ref, win_t, wout, wout_t):
    new = lax.broadcasted_iota(jnp.int32, (HID, 1), 0)
    old = lax.broadcasted_iota(jnp.int32, (HID, HID), 1)
    core = new // 384
    chip = (new - core * 384) // 48
    within = new - core * 384 - chip * 48
    table = within // 3
    place = table * 48 + (2 * chip + core) * 3 + (within - table * 3)
    perm = (old == place).astype(F32).astype(BF16)
    win_t[...] = mm(perm, win_ref[...], NT).astype(BF16)
    wout[...] = (0.5 * mm(perm, wout_ref[...], NT)).astype(BF16)
    wout_t[...] = (0.5 * mm(wout_ref[...], perm, NT)).astype(BF16)


def feed_forward(step, cot_ref, turn0, turn1, win_t, wout, wout_t, tok, cot, sums, out_buf):
    for j in range(DROWS):
        at = step * DROWS + j
        tok[128 * j : 128 * j + FEATS, 0:128] = turn0[pl.ds(at, FEATS, stride=STRIDE), :].astype(BF16)
        tok[128 * j : 128 * j + FEATS, 128:192] = turn1[pl.ds(at, FEATS, stride=STRIDE), 0:64].astype(BF16)
        cot[:, 128 * j : 128 * j + FEATS] = cot_ref[at]
    x = tok[...]
    c = cot[...]
    total = mm(eye(E), x, NT)
    waiting = []
    for n in range(HID // HBLOCK + 1):
        if n < HID // HBLOCK:
            rows = pl.ds(HBLOCK * n, HBLOCK)
            waiting.append((mm(win_t[rows, :], x, NT), mm(wout[rows, :], c)))
        if n:
            pre, dact = waiting.pop(0)
            begin = HBLOCK * (n - 1)
            rows = pl.ds(begin, HBLOCK)
            u = pre * math.sqrt(0.5)
            twice = lax.erf(u) + 1.0
            act = (pre * twice).astype(BF16)
            slope = twice + u * jnp.exp2(math.log2(2.0 / math.sqrt(math.pi)) - (u * u) * math.log2(math.e))
            dpre = (dact * slope).astype(BF16)
            sums[0, rows, :] += mm(dpre, x)
            sums[1, rows, :] += mm(act, c, NT)
            total = total + mm(wout_t[:, begin : begin + HBLOCK], act)
    for j in range(DROWS):
        out_buf[step * DROWS + j] = total[:, 128 * j : 128 * j + FEATS].astype(BF16)


FBLOCK = 4
TILES = 11
CHUNK = 256
LAG = 2


def layer_kernel(
    remote,
    feat_count,
    train_count,
    x_hbm,
    fw_ref,
    fproj_ref,
    rw_ref,
    rproj_ref,
    win_ref,
    wout_ref,
    cot_hbm,
    out_hbm,
    grad_in_ref,
    grad_out_ref,
    fwide,
    fproj,
    rwide,
    rproj,
    tok,
    kept,
    qkv,
    vals0,
    vals1,
    att,
    turn0,
    turn1,
    send,
    cols,
    rq,
    rkv,
    keys,
    vals,
    ratt,
    done,
    x_ref,
    cot_ref,
    normed,
    win_t,
    wout,
    wout_t,
    dtok,
    dcot,
    sums,
    out_buf,
    part,
    pair,
    half_sum,
    got_chips,
    lined,
    row,
    got_tables,
    send_sem,
    cols_sem,
    send2_sem,
    recv2_sem,
    local_sem,
    sums_sem,
):
    me = lax.axis_index("cells") if remote else 0
    first_x = pltpu.make_async_copy(x_hbm.at[0:8], x_ref.at[0:8], local_sem.at[0])
    rest_x = pltpu.make_async_copy(x_hbm.at[8:LOCAL], x_ref.at[8:LOCAL], local_sem.at[1])
    all_cot = pltpu.make_async_copy(cot_hbm, cot_ref, local_sem.at[2])
    first_x.start()
    rest_x.start()
    all_cot.start()
    if remote:
        greet(("cells", "tables"))
    spread_weights(fw_ref, fwide, fproj_ref, fproj)
    ident = eye(FEATS)
    tok[:, 192:256] = jnp.zeros((FBLOCK * FEATS, 64), F32)
    lane = lax.broadcasted_iota(jnp.int32, (1, 128), 1)
    bias = jnp.where(lane < feat_count[0], 0.0, NEG).astype(F32)
    for ref, heads in ((vals0, range(4)), (vals1, range(4, 6))):
        ref[...] = jnp.zeros(ref.shape, BF16)
        for j in range(FBLOCK):
            for i, h in enumerate(heads):
                ref[j, 128 * i : 128 * i + FEATS, 128:256] = jnp.broadcast_to(ones_mask(h), (FEATS, 128))
    zero_pad = jnp.zeros((128 - FEATS, 128), BF16)

    def project(step):
        for j in range(FBLOCK):
            tok[pl.ds(FEATS * j, FEATS), 0:192] = mm(ident, x_ref[step * FBLOCK + j], NT)
        qkv[...] = mm(tok[...].astype(BF16), fwide[...])

    tiles_of_heads = ((range(4), vals0), (range(4, 6), vals1))

    def score_rows():
        scores = []
        for j in range(FBLOCK):
            rows = pl.ds(FEATS * j, FEATS)
            for tile, (heads, ref) in enumerate(tiles_of_heads):
                at = 128 * tile
                q = (qkv[rows, at : at + 128] * QSCALE).astype(BF16)
                k = qkv[rows, 256 + at : 384 + at].astype(BF16)
                v = qkv[rows, 512 + at : 640 + at].astype(BF16)
                pieces = []
                for i, h in enumerate(heads):
                    pieces += [k * head_mask(h), zero_pad]
                    ref[j, 128 * i : 128 * i + FEATS, 0:128] = v * head_mask(h)
                scores.append(mm(q, jnp.concatenate(pieces, axis=0), NT))
        return scores

    def attend(scores):
        for j in range(FBLOCK):
            rows = pl.ds(FEATS * j, FEATS)
            for tile, (heads, ref) in enumerate(tiles_of_heads):
                probs = []
                for i, h in enumerate(heads):
                    s = scores[2 * j + tile][:, 128 * i : 128 * i + 128] + bias
                    probs.append(jnp.exp2(s - jnp.max(s, axis=-1, keepdims=True)).astype(BF16))
                got = mm(jnp.concatenate(probs, axis=1), ref[j])
                att[rows, 128 * tile : 128 * tile + 128] = (got[:, :128] / got[:, 128:]).astype(BF16)

    def finish(step):
        mixed = mm(att[...], fproj[...])
        low, high = layer_norm(kept[:, 0:128] + mixed[:, 0:128], kept[:, 128:256] + mixed[:, 128:256])
        for j in range(FBLOCK):
            at = step * FBLOCK + j
            turn0[pl.ds(at, FEATS, stride=STRIDE), :] = low[FEATS * j : FEATS * j + FEATS]
            turn1[pl.ds(at, FEATS, stride=STRIDE), :] = high[FEATS * j : FEATS * j + FEATS]

    def blocks(step, _):
        scores = score_rows()
        finish(step - 2)
        kept[...] = tok[...]
        project(step)
        attend(scores)
        return 0

    def pack(p, group, half):
        def rows_of(ref, f):
            return ref[pl.ds(pl.multiple_of((p * OWN + f) * STRIDE + 16 * half, 8), 16), :]

        f = 2 * group
        at = 3 * group
        send[p, half, at] = rows_of(turn0, f).astype(BF16)
        high = rows_of(turn1, f)
        if f + 1 < OWN:
            at += 1
            send[p, half, at] = rows_of(turn0, f + 1).astype(BF16)
            high = high + pltpu.roll(rows_of(turn1, f + 1), 64, 1)
        send[p, half, at + 1] = high.astype(BF16)

    def pass_on(source, target, k, axis, p, send_s, recv_s):
        if not remote:
            pltpu.make_async_copy(source, target, recv_s).start()
            return

        @pl.when(k == 0)
        def _():
            pltpu.make_async_copy(source, target, recv_s).start()

        @pl.when(k != 0)
        def _():
            pltpu.make_async_remote_copy(
                src_ref=source,
                dst_ref=target,
                send_sem=send_s,
                recv_sem=recv_s,
                device_id={axis: p},
                device_id_type=MESH,
            ).start()

    def place(p):
        return me if remote else p

    first_x.wait()
    project(0)
    scores = score_rows()
    kept[...] = tok[...]
    project(1)
    attend(scores)
    rest_x.wait()
    lax.fori_loop(2, 2 + 16 // FBLOCK, blocks, 0)
    if remote:
        await_peers(("cells", "tables"))

    def first_half(k, _):
        p = lax.rem(me + k, PEERS)
        for group in range(4):
            pack(p, group, 0)
        pass_on(
            send.at[p, 0],
            cols.at[0, place(p)],
            k,
            "cells",
            p,
            send_sem,
            cols_sem.at[4],
        )
        return 0

    lax.fori_loop(0, PEERS, first_half, 0)
    lax.fori_loop(2 + 16 // FBLOCK, 32 // FBLOCK, blocks, 0)
    scores = score_rows()
    finish(32 // FBLOCK - 2)
    kept[...] = tok[...]
    attend(scores)
    finish(32 // FBLOCK - 1)
    for group in range(4):
        tiles = pl.ds(3 * group, min(3, TILES - 3 * group))

        def second_half(k, _):
            p = lax.rem(me + k, PEERS)
            pack(p, group, 1)
            pass_on(
                send.at[p, 1, tiles],
                cols.at[1, place(p), tiles],
                k,
                "cells",
                p,
                send_sem,
                cols_sem.at[group],
            )
            return 0

        lax.fori_loop(0, PEERS, second_half, 0)

    spread_weights(rw_ref, rwide, rproj_ref, rproj)
    lane = lax.broadcasted_iota(jnp.int32, (1, KEYS), 1)
    rbias = jnp.where(lane < train_count[0], 0.0, NEG).astype(F32)
    for h in range(HEADS):
        vals[KEYS * h : KEYS * h + KEYS, 128:256] = jnp.broadcast_to(ones_mask(h), (KEYS, 128))
    half_lane = lax.broadcasted_iota(jnp.int32, (1, 128), 1) < 64
    order_hidden(win_ref, wout_ref, win_t, wout, wout_t)
    sums[...] = jnp.zeros(sums.shape, F32)
    dtok[...] = jnp.zeros(dtok.shape, BF16)
    dcot[...] = jnp.zeros(dcot.shape, BF16)

    def column(f, _):
        @pl.when(f == 0)
        def _():
            ref = cols.at[0]
            pltpu.make_async_copy(ref, ref, cols_sem.at[4]).wait()

        for group in range(4):

            @pl.when(f == 2 * group)
            def _():
                ref = cols.at[1, :, pl.ds(3 * group, min(3, TILES - 3 * group))]
                pltpu.make_async_copy(ref, ref, cols_sem.at[group]).wait()

        odd = lax.rem(f, 2)
        at = 3 * (f // 2)

        def tokens(tile):
            return jnp.stack([cols[0, :, tile], cols[1, :, tile]], axis=1).reshape(ROWS, 128)

        low = tokens(at + odd)
        high = tokens(jnp.minimum(at + 2, TILES - 1)).astype(F32)
        high = jnp.where(half_lane, pltpu.roll(high, 64 * odd, 1), 0.0)
        x = jnp.concatenate([low, high.astype(BF16)], axis=1)
        rq[...] = (mm(x, rwide[:, 0:256]) * QSCALE).astype(BF16)
        rkv[...] = mm(x[0:KEYS], rwide[:, 256:768]).astype(BF16)
        for h in range(HEADS):
            at = 128 * (h // 4)
            rows = pl.ds(KEYS * h, KEYS)
            keys[rows, :] = rkv[:, at : at + 128] * head_mask(h)
            vals[rows, 0:128] = rkv[:, 256 + at : 384 + at] * head_mask(h)

        def score_pair(begin, first):
            at = 128 * (first // 4)
            return mm(rq[begin : begin + CHUNK, at : at + 128], keys[pl.ds(KEYS * first, 2 * KEYS), :], NT)

        def value_pair(first, score):
            probs = []
            for i in range(2):
                s = score[:, KEYS * i : KEYS * i + KEYS] + rbias
                probs.append(jnp.exp2(s - jnp.max(s, axis=-1, keepdims=True)).astype(BF16))
            return mm(jnp.concatenate(probs, axis=1), vals[pl.ds(KEYS * first, 2 * KEYS), :])

        units = [(begin, first) for begin in range(0, ROWS, CHUNK) for first in (0, 2, 4)]
        waiting = []
        got = None
        for n in range(len(units) + LAG):
            if n < len(units):
                waiting.append(score_pair(*units[n]))
            if n >= LAG:
                begin, first = units[n - LAG]
                more = value_pair(first, waiting.pop(0))
                got = more if first != 2 else got + more
                if first:
                    at = 128 * (first // 4)
                    ratt[begin : begin + CHUNK, at : at + 128] = (got[:, :128] / got[:, 128:]).astype(BF16)
        mixed = mm(ratt[...], rproj[...])
        low, high = layer_norm(low.astype(F32) + mixed[:, 0:128], high + mixed[:, 128:256])
        done[f, :, 0:32, :] = low.astype(BF16).reshape(PEERS, 32, 128)
        high = high.reshape(PEERS, 2, 16, 128)
        high = high[:, 0] + pltpu.roll(high[:, 1].reshape(PEERS * 16, 128), 64, 1).reshape(PEERS, 16, 128)
        done[f, :, 32:48, :] = high.astype(BF16)

        def to_peer(k, _):
            p = lax.rem(me + k, PEERS)
            pass_on(
                done.at[f, p],
                normed.at[f, place(p)],
                k,
                "cells",
                p,
                send2_sem,
                recv2_sem.at[f],
            )
            return 0

        return lax.fori_loop(0, PEERS, to_peer, 0)

    lax.fori_loop(0, OWN, column, 0)

    def unpack(f, _):
        pltpu.make_async_copy(normed.at[f], normed.at[f], recv2_sem.at[f]).wait()
        for p in range(PEERS):
            at = pl.multiple_of((p * OWN + f) * STRIDE, 8)
            turn0[pl.ds(at, LOCAL), :] = normed[f, p, 0:32, :].astype(F32)
            high = normed[f, p, 32:48, :].astype(F32)
            turn1[pl.ds(at, 16), :] = high
            turn1[pl.ds(at + 16, 16), :] = pltpu.roll(high, 64, 1)
        return 0

    all_cot.wait()
    lax.fori_loop(0, OWN, unpack, 0)

    def feed(step, _):
        feed_forward(step, cot_ref, turn0, turn1, win_t, wout, wout_t, dtok, dcot, sums, out_buf)
        rows = pl.ds(step * DROWS, DROWS)
        pltpu.make_async_copy(out_buf.at[rows], out_hbm.at[rows], local_sem.at[3]).start()
        return 0

    lax.fori_loop(0, LOCAL // DROWS, feed, 0)
    factor = 1.0 / math.sqrt(16 * ROWS * FEATS)
    part[0] = (sums[0, :, 0:128] * factor).astype(BF16)
    part[1] = (sums[1, :, 0:128] * (0.5 * factor)).astype(BF16)
    part[2, :, 0:64] = (sums[0, :, 128:192] * factor).astype(BF16)
    part[2, :, 64:128] = (sums[1, :, 128:192] * (0.5 * factor)).astype(BF16)

    table = lax.axis_index("tables") if remote else 0
    chip = me // 2
    core = me - 2 * chip
    theirs = pl.ds(pl.multiple_of((1 - core) * 384, 384), 384)
    mine = pl.ds(pl.multiple_of(core * 384, 384), 384)
    if remote:
        swap = pltpu.make_async_remote_copy(
            src_ref=part.at[:, theirs, :],
            dst_ref=pair,
            send_sem=sums_sem.at[0],
            recv_sem=sums_sem.at[1],
            device_id={"cells": 2 * chip + 1 - core},
            device_id_type=MESH,
        )
    else:
        swap = pltpu.make_async_copy(part.at[:, theirs, :], pair, sums_sem.at[1])
    swap.start()
    swap.wait()
    for t in range(3):
        half_sum[t] = (part[t, mine, :].astype(F32) + pair[t].astype(F32)).astype(BF16)

    def to_chip(k, _):
        p = lax.rem(chip + k, CHIPS)
        source = half_sum.at[:, pl.ds(pl.multiple_of(48 * p, 16), 48), :]
        target = got_chips.at[chip if remote else p]
        pass_on(source, target, k, "cells", 2 * p + core, sums_sem.at[2], sums_sem.at[3])
        return 0

    lax.fori_loop(0, CHIPS, to_chip, 0)
    lined[...] = jnp.zeros(lined.shape, F32)
    pltpu.make_async_copy(got_chips, got_chips, sums_sem.at[3]).wait()
    total = got_chips[0].astype(F32)
    for p in range(1, CHIPS):
        total = total + got_chips[p].astype(F32)
    for t in range(PEERS):
        for i in range(3):
            lined[t, 4 * i : 4 * i + 3, :] = total[i, 3 * t : 3 * t + 3, :]
    row[...] = lined[...].astype(BF16)

    def to_table(k, _):
        p = lax.rem(table + k, PEERS)
        pass_on(row.at[p], got_tables.at[table if remote else p], k, "tables", p, sums_sem.at[4], sums_sem.at[5])
        return 0

    lax.fori_loop(0, PEERS, to_table, 0)
    pltpu.make_async_copy(out_buf, out_hbm, local_sem.at[3]).wait()
    if remote:
        sent = send.at[pl.ds(0, PEERS - 1)]
        pltpu.make_async_copy(sent, sent, send_sem).wait()
        sent = normed.at[:, pl.ds(0, PEERS - 1)]
        pltpu.make_async_copy(sent, sent, send2_sem).wait()
        sent = got_chips.at[pl.ds(0, CHIPS - 1)]
        pltpu.make_async_copy(sent, sent, sums_sem.at[2]).wait()
        sent = got_tables.at[pl.ds(0, PEERS - 1)]
        pltpu.make_async_copy(sent, sent, sums_sem.at[4]).wait()
    pltpu.make_async_copy(got_tables, got_tables, sums_sem.at[5]).wait()
    final = got_tables[0].astype(F32)
    for t in range(1, PEERS):
        final = final + got_tables[t].astype(F32)
    grad_in_ref[:, 0:128] = final[0:3, :]
    grad_in_ref[:, 128:192] = final[8:11, 0:64]
    grad_out_ref[:, 0:128] = final[4:7, :]
    grad_out_ref[:, 128:192] = final[8:11, 64:128]


def whole_layer(
    x_t, feat_count, train_count, feat_qkv, feat_proj, row_qkv, row_proj, w_in, w_out_t, cot_t, remote=True
):
    vmem = pl.BlockSpec(memory_space=pltpu.VMEM)
    smem = pl.BlockSpec(memory_space=pltpu.SMEM)
    hbm = pl.BlockSpec(memory_space=pl.ANY)
    return pl.pallas_call(
        functools.partial(layer_kernel, remote),
        name="layer",
        out_shape=(
            jax.ShapeDtypeStruct((LOCAL, E, FEATS), BF16),
            jax.ShapeDtypeStruct((3, E), F32),
            jax.ShapeDtypeStruct((3, E), F32),
        ),
        in_specs=[smem, smem, hbm] + [vmem] * 6 + [hbm],
        out_specs=(hbm, vmem, vmem),
        scratch_shapes=[
            pltpu.VMEM((256, 768), BF16),
            pltpu.VMEM((256, 256), BF16),
            pltpu.VMEM((256, 768), BF16),
            pltpu.VMEM((256, 256), BF16),
            pltpu.VMEM((FBLOCK * FEATS, 256), F32),
            pltpu.VMEM((FBLOCK * FEATS, 256), F32),
            pltpu.VMEM((FBLOCK * FEATS, 768), F32),
            pltpu.VMEM((FBLOCK, 512, 256), BF16),
            pltpu.VMEM((FBLOCK, 256, 256), BF16),
            pltpu.VMEM((FBLOCK * FEATS, 256), BF16),
            pltpu.VMEM((FEATS * STRIDE, 128), F32),
            pltpu.VMEM((FEATS * STRIDE, 128), F32),
            pltpu.VMEM((PEERS, 2, TILES, 16, 128), BF16),
            pltpu.VMEM((2, PEERS, TILES, 16, 128), BF16),
            pltpu.VMEM((ROWS, 256), BF16),
            pltpu.VMEM((KEYS, 512), BF16),
            pltpu.VMEM((HEADS * KEYS, 128), BF16),
            pltpu.VMEM((HEADS * KEYS, 256), BF16),
            pltpu.VMEM((ROWS, 256), BF16),
            pltpu.VMEM((OWN, PEERS, 48, 128), BF16),
            pltpu.VMEM((LOCAL, E, FEATS), BF16),
            pltpu.VMEM((LOCAL, E, FEATS), BF16),
            pltpu.VMEM((OWN, PEERS, 48, 128), BF16),
            pltpu.VMEM((HID, E), BF16),
            pltpu.VMEM((HID, E), BF16),
            pltpu.VMEM((E, HID), BF16),
            pltpu.VMEM((DTOK, E), BF16),
            pltpu.VMEM((E, DTOK), BF16),
            pltpu.VMEM((2, HID, E), F32),
            pltpu.VMEM((LOCAL, E, FEATS), BF16),
            pltpu.VMEM((3, HID, 128), BF16),
            pltpu.VMEM((3, 384, 128), BF16),
            pltpu.VMEM((3, 384, 128), BF16),
            pltpu.VMEM((CHIPS, 3, 48, 128), BF16),
            pltpu.VMEM((PEERS, 16, 128), F32),
            pltpu.VMEM((PEERS, 16, 128), BF16),
            pltpu.VMEM((PEERS, 16, 128), BF16),
            pltpu.SemaphoreType.DMA,
            pltpu.SemaphoreType.DMA((5,)),
            pltpu.SemaphoreType.DMA,
            pltpu.SemaphoreType.DMA((OWN,)),
            pltpu.SemaphoreType.DMA((4,)),
            pltpu.SemaphoreType.DMA((6,)),
        ],
        compiler_params=pltpu.CompilerParams(
            collective_id=0 if remote else None, has_side_effects=True, vmem_limit_bytes=VMEM_LIMIT
        ),
    )(feat_count, train_count, x_t, feat_qkv, feat_proj, row_qkv, row_proj, w_in, w_out_t, cot_t)


def per_device(
    cells_in, train_count, feat_count, feat_qkv, feat_proj, row_qkv, row_proj, w_in, w_out, cotangent
):
    x_t = jnp.swapaxes(cells_in[0], 1, 2)
    cot_t = jnp.swapaxes(cotangent[0], 1, 2)
    out_t, grad_in, grad_out = whole_layer(
        x_t, feat_count, train_count, feat_qkv, feat_proj, row_qkv, row_proj, w_in, w_out.T, cot_t
    )
    return (jnp.swapaxes(out_t, 1, 2)[None], grad_in.T, grad_out)


def solution(mesh):
    return jax.shard_map(
        per_device,
        mesh=mesh,
        in_specs=(
            P("tables", "cells", None, None),
            P("tables"),
            P("tables"),
            P(),
            P(),
            P(),
            P(),
            P(),
            P(),
            P("tables", "cells", None, None),
        ),
        out_specs=(
            P("tables", "cells", None, None),
            P(None, ("tables", "cells")),
            P(("tables", "cells"), None),
        ),
        check_vma=False,
    )
```

```python
import functools
import math

import jax
import jax.numpy as jnp
from jax import lax
from jax.experimental import pallas as pl
from jax.experimental.pallas import tpu as pltpu
from jax.sharding import PartitionSpec as P

HEADS = 6
HEAD_DIM = 32
E = 192
HID = 768
FEATS = 112
ROWS = 512
LOCAL = 32
PEERS = 16
OWN = 7
KEYS = 384
STRIDE = 40
F32 = jnp.float32
BF16 = jnp.bfloat16
NEG = -1e30
QSCALE = math.log2(math.e) / math.sqrt(HEAD_DIM)
VMEM_LIMIT = 53 * 1024 * 1024
MESH = pl.DeviceIdType.MESH

NN = (((1,), (0,)), ((), ()))
NT = (((1,), (1,)), ((), ()))


def mm(a, b, dims=NN):
    return lax.dot_general(a, b, dims, preferred_element_type=F32)


def eye(n):
    r = lax.broadcasted_iota(jnp.int32, (n, n), 0)
    c = lax.broadcasted_iota(jnp.int32, (n, n), 1)
    return (r == c).astype(F32).astype(BF16)


def head_mask(head):
    lane = lax.broadcasted_iota(jnp.int32, (1, 128), 1)
    low = 32 * (head % 4)
    return ((lane >= low) & (lane < low + 32)).astype(F32).astype(BF16)


def ones_mask(head):
    lane = lax.broadcasted_iota(jnp.int32, (1, 128), 1)
    low = 32 * (head % 4)
    high = 128 if head == 5 else low + 32
    return ((lane >= low) & (lane < high)).astype(F32).astype(BF16)


def spread_weights(w_ref, wide_ref, proj_ref, proj_wide):
    wide_ref[...] = jnp.zeros(wide_ref.shape, BF16)
    for part in range(3):
        wide_ref[0:192, 256 * part : 256 * part + 192] = w_ref[:, 192 * part : 192 * part + 192]
    proj_wide[...] = jnp.zeros(proj_wide.shape, BF16)
    proj_wide[0:192, 0:192] = proj_ref[...]


def layer_norm(low, high):
    mean = (jnp.sum(low, axis=-1, keepdims=True) + jnp.sum(high, axis=-1, keepdims=True)) * (1.0 / E)
    low = low - mean
    half = lax.broadcasted_iota(jnp.int32, (1, 128), 1) < 64
    high = jnp.where(half, high - mean, 0.0)
    var = jnp.sum(low * low + high * high, axis=-1, keepdims=True) * (1.0 / E)
    scale = lax.rsqrt(var + 1e-05)
    return low * scale, high * scale


def greet(axes):
    barrier = pltpu.get_barrier_semaphore()
    for axis in axes:
        me = lax.axis_index(axis)

        @pl.loop(1, PEERS)
        def _(k):
            pl.semaphore_signal(
                barrier, inc=1, device_id={axis: lax.rem(me + k, PEERS)}, device_id_type=MESH
            )


def await_peers(axes):
    pl.semaphore_wait(pltpu.get_barrier_semaphore(), (PEERS - 1) * len(axes))


DROWS = 4
DTOK = DROWS * 128
HBLOCK = 256
BLOCKS = 2
AHEAD = 1
STEPS = LOCAL // DROWS
CHIPS = PEERS // 2


def order_hidden(win_ref, wout_ref, win_t, wout, wout_t):
    new = lax.broadcasted_iota(jnp.int32, (HID, 1), 0)
    old = lax.broadcasted_iota(jnp.int32, (HID, HID), 1)
    core = new // 384
    chip = (new - core * 384) // 48
    within = new - core * 384 - chip * 48
    table = within // 3
    place = table * 48 + (2 * chip + core) * 3 + (within - table * 3)
    perm = (old == place).astype(F32).astype(BF16)
    win_t[...] = mm(perm, win_ref[...], NT).astype(BF16)
    wout[...] = (0.5 * mm(perm, wout_ref[...], NT)).astype(BF16)
    wout_t[...] = (0.5 * mm(wout_ref[...], perm, NT)).astype(BF16)


def feed_forward(first, cot_ref, turn0, turn1, win_t, wout, toks, acts, cot, sums):
    units = []
    for b in range(BLOCKS):
        for j in range(DROWS):
            at = (first + b) * DROWS + j
            rows = pl.ds(128 * j, FEATS)
            toks[first + b, rows, 0:128] = turn0[pl.ds(at, FEATS, stride=STRIDE), :].astype(BF16)
            toks[first + b, rows, 128:192] = turn1[pl.ds(at, FEATS, stride=STRIDE), 0:64].astype(BF16)
            cot[b, :, 128 * j : 128 * j + FEATS] = cot_ref[at]
        units += [(b, begin) for begin in range(0, HID, HBLOCK)]
    waiting = []
    for n in range(len(units) + AHEAD):
        if n < len(units):
            b, begin = units[n]
            rows = pl.ds(begin, HBLOCK)
            waiting.append((mm(win_t[rows, :], toks[first + b], NT), mm(wout[rows, :], cot[b])))
        if n >= AHEAD:
            b, begin = units[n - AHEAD]
            rows = pl.ds(begin, HBLOCK)
            pre, dact = waiting.pop(0)
            u = pre * math.sqrt(0.5)
            twice = lax.erf(u) + 1.0
            act = (pre * twice).astype(BF16)
            slope = twice + u * jnp.exp2(math.log2(2.0 / math.sqrt(math.pi)) - (u * u) * math.log2(math.e))
            dpre = (dact * slope).astype(BF16)
            acts[first + b, rows, :] = act
            sums[0, rows, :] += mm(dpre, toks[first + b])
            sums[1, rows, :] += mm(act, cot[b], NT)


def output_cells(step, wout_t, toks, acts, out_ref):
    total = mm(eye(E), toks[step], NT) + mm(wout_t[...], acts[step])
    for j in range(DROWS):
        out_ref[step * DROWS + j] = total[:, 128 * j : 128 * j + FEATS].astype(BF16)


FBLOCK = 4
TILES = 11
CHUNK = 256
LAG = 2


def layer_kernel(
    remote,
    feat_count,
    train_count,
    x_hbm,
    fw_ref,
    fproj_ref,
    rw_ref,
    rproj_ref,
    win_ref,
    wout_ref,
    cot_hbm,
    out_ref,
    grad_in_ref,
    grad_out_ref,
    fwide,
    fproj,
    rwide,
    rproj,
    tok,
    kept,
    qkv,
    vals0,
    vals1,
    att,
    turn0,
    turn1,
    send,
    cols,
    rq,
    rkv,
    keys,
    vals,
    ratt,
    done,
    x_ref,
    cot_ref,
    normed,
    win_t,
    wout,
    wout_t,
    toks,
    acts,
    dcot,
    sums,
    part,
    pair,
    half_sum,
    got_chips,
    lined,
    row,
    got_tables,
    send_sem,
    cols_sem,
    send2_sem,
    recv2_sem,
    local_sem,
    sums_sem,
):
    me = lax.axis_index("cells") if remote else 0
    first_x = pltpu.make_async_copy(x_hbm.at[0:8], x_ref.at[0:8], local_sem.at[0])
    rest_x = pltpu.make_async_copy(x_hbm.at[8:LOCAL], x_ref.at[8:LOCAL], local_sem.at[1])
    all_cot = pltpu.make_async_copy(cot_hbm, cot_ref, local_sem.at[2])
    first_x.start()
    rest_x.start()
    all_cot.start()
    if remote:
        greet(("cells", "tables"))
    spread_weights(fw_ref, fwide, fproj_ref, fproj)
    ident = eye(FEATS)
    tok[:, 192:256] = jnp.zeros((FBLOCK * FEATS, 64), F32)
    lane = lax.broadcasted_iota(jnp.int32, (1, 128), 1)
    bias = jnp.where(lane < feat_count[0], 0.0, NEG).astype(F32)
    for ref, heads in ((vals0, range(4)), (vals1, range(4, 6))):
        ref[...] = jnp.zeros(ref.shape, BF16)
        for j in range(FBLOCK):
            for i, h in enumerate(heads):
                ref[j, 128 * i : 128 * i + FEATS, 128:256] = jnp.broadcast_to(ones_mask(h), (FEATS, 128))
    zero_pad = jnp.zeros((128 - FEATS, 128), BF16)

    def project(step):
        for j in range(FBLOCK):
            tok[pl.ds(FEATS * j, FEATS), 0:192] = mm(ident, x_ref[step * FBLOCK + j], NT)
        qkv[...] = mm(tok[...].astype(BF16), fwide[...])

    tiles_of_heads = ((range(4), vals0), (range(4, 6), vals1))

    def score_rows():
        scores = []
        for j in range(FBLOCK):
            rows = pl.ds(FEATS * j, FEATS)
            for tile, (heads, ref) in enumerate(tiles_of_heads):
                at = 128 * tile
                q = (qkv[rows, at : at + 128] * QSCALE).astype(BF16)
                k = qkv[rows, 256 + at : 384 + at].astype(BF16)
                v = qkv[rows, 512 + at : 640 + at].astype(BF16)
                pieces = []
                for i, h in enumerate(heads):
                    pieces += [k * head_mask(h), zero_pad]
                    ref[j, 128 * i : 128 * i + FEATS, 0:128] = v * head_mask(h)
                scores.append(mm(q, jnp.concatenate(pieces, axis=0), NT))
        return scores

    def attend(scores):
        for j in range(FBLOCK):
            rows = pl.ds(FEATS * j, FEATS)
            for tile, (heads, ref) in enumerate(tiles_of_heads):
                probs = []
                for i, h in enumerate(heads):
                    s = scores[2 * j + tile][:, 128 * i : 128 * i + 128] + bias
                    probs.append(jnp.exp2(s - jnp.max(s, axis=-1, keepdims=True)).astype(BF16))
                got = mm(jnp.concatenate(probs, axis=1), ref[j])
                att[rows, 128 * tile : 128 * tile + 128] = (got[:, :128] / got[:, 128:]).astype(BF16)

    def finish(step):
        mixed = mm(att[...], fproj[...])
        low, high = layer_norm(kept[:, 0:128] + mixed[:, 0:128], kept[:, 128:256] + mixed[:, 128:256])
        for j in range(FBLOCK):
            at = step * FBLOCK + j
            turn0[pl.ds(at, FEATS, stride=STRIDE), :] = low[FEATS * j : FEATS * j + FEATS]
            turn1[pl.ds(at, FEATS, stride=STRIDE), :] = high[FEATS * j : FEATS * j + FEATS]

    def blocks(step, _):
        scores = score_rows()
        finish(step - 2)
        kept[...] = tok[...]
        project(step)
        attend(scores)
        return 0

    def pack(p, group, half):
        def rows_of(ref, f):
            return ref[pl.ds(pl.multiple_of((p * OWN + f) * STRIDE + 16 * half, 8), 16), :]

        f = 2 * group
        at = 3 * group
        send[p, half, at] = rows_of(turn0, f).astype(BF16)
        high = rows_of(turn1, f)
        if f + 1 < OWN:
            at += 1
            send[p, half, at] = rows_of(turn0, f + 1).astype(BF16)
            high = high + pltpu.roll(rows_of(turn1, f + 1), 64, 1)
        send[p, half, at + 1] = high.astype(BF16)

    def pass_on(source, target, k, axis, p, send_s, recv_s):
        if not remote:
            pltpu.make_async_copy(source, target, recv_s).start()
            return

        @pl.when(k == 0)
        def _():
            pltpu.make_async_copy(source, target, recv_s).start()

        @pl.when(k != 0)
        def _():
            pltpu.make_async_remote_copy(
                src_ref=source,
                dst_ref=target,
                send_sem=send_s,
                recv_sem=recv_s,
                device_id={axis: p},
                device_id_type=MESH,
            ).start()

    def place(p):
        return me if remote else p

    first_x.wait()
    project(0)
    scores = score_rows()
    kept[...] = tok[...]
    project(1)
    attend(scores)
    rest_x.wait()
    lax.fori_loop(2, 2 + 16 // FBLOCK, blocks, 0)
    if remote:
        await_peers(("cells", "tables"))

    def first_half(k, _):
        p = lax.rem(me + k, PEERS)
        for group in range(4):
            pack(p, group, 0)
        pass_on(
            send.at[p, 0],
            cols.at[0, place(p)],
            k,
            "cells",
            p,
            send_sem,
            cols_sem.at[4],
        )
        return 0

    lax.fori_loop(0, PEERS, first_half, 0)
    lax.fori_loop(2 + 16 // FBLOCK, 32 // FBLOCK, blocks, 0)
    scores = score_rows()
    finish(32 // FBLOCK - 2)
    kept[...] = tok[...]
    attend(scores)
    finish(32 // FBLOCK - 1)
    for group in range(4):
        tiles = pl.ds(3 * group, min(3, TILES - 3 * group))

        def second_half(k, _):
            p = lax.rem(me + k, PEERS)
            pack(p, group, 1)
            pass_on(
                send.at[p, 1, tiles],
                cols.at[1, place(p), tiles],
                k,
                "cells",
                p,
                send_sem,
                cols_sem.at[group],
            )
            return 0

        lax.fori_loop(0, PEERS, second_half, 0)

    spread_weights(rw_ref, rwide, rproj_ref, rproj)
    lane = lax.broadcasted_iota(jnp.int32, (1, KEYS), 1)
    rbias = jnp.where(lane < train_count[0], 0.0, NEG).astype(F32)
    for h in range(HEADS):
        vals[KEYS * h : KEYS * h + KEYS, 128:256] = jnp.broadcast_to(ones_mask(h), (KEYS, 128))
    half_lane = lax.broadcasted_iota(jnp.int32, (1, 128), 1) < 64
    order_hidden(win_ref, wout_ref, win_t, wout, wout_t)
    sums[...] = jnp.zeros(sums.shape, F32)
    toks[...] = jnp.zeros(toks.shape, BF16)
    dcot[...] = jnp.zeros(dcot.shape, BF16)

    def column(f, _):
        @pl.when(f == 0)
        def _():
            ref = cols.at[0]
            pltpu.make_async_copy(ref, ref, cols_sem.at[4]).wait()

        for group in range(4):

            @pl.when(f == 2 * group)
            def _():
                ref = cols.at[1, :, pl.ds(3 * group, min(3, TILES - 3 * group))]
                pltpu.make_async_copy(ref, ref, cols_sem.at[group]).wait()

        odd = lax.rem(f, 2)
        at = 3 * (f // 2)

        def tokens(tile):
            return jnp.stack([cols[0, :, tile], cols[1, :, tile]], axis=1).reshape(ROWS, 128)

        low = tokens(at + odd)
        high = tokens(jnp.minimum(at + 2, TILES - 1)).astype(F32)
        high = jnp.where(half_lane, pltpu.roll(high, 64 * odd, 1), 0.0)
        x = jnp.concatenate([low, high.astype(BF16)], axis=1)
        rq[...] = (mm(x, rwide[:, 0:256]) * QSCALE).astype(BF16)
        rkv[...] = mm(x[0:KEYS], rwide[:, 256:768]).astype(BF16)
        for h in range(HEADS):
            at = 128 * (h // 4)
            rows = pl.ds(KEYS * h, KEYS)
            keys[rows, :] = rkv[:, at : at + 128] * head_mask(h)
            vals[rows, 0:128] = rkv[:, 256 + at : 384 + at] * head_mask(h)

        def score_pair(begin, first):
            at = 128 * (first // 4)
            return mm(rq[begin : begin + CHUNK, at : at + 128], keys[pl.ds(KEYS * first, 2 * KEYS), :], NT)

        def value_pair(first, score):
            probs = []
            for i in range(2):
                s = score[:, KEYS * i : KEYS * i + KEYS] + rbias
                probs.append(jnp.exp2(s - jnp.max(s, axis=-1, keepdims=True)).astype(BF16))
            return mm(jnp.concatenate(probs, axis=1), vals[pl.ds(KEYS * first, 2 * KEYS), :])

        units = [(begin, first) for begin in range(0, ROWS, CHUNK) for first in (0, 2, 4)]
        waiting = []
        got = None
        for n in range(len(units) + LAG):
            if n < len(units):
                waiting.append(score_pair(*units[n]))
            if n >= LAG:
                begin, first = units[n - LAG]
                more = value_pair(first, waiting.pop(0))
                got = more if first != 2 else got + more
                if first:
                    at = 128 * (first // 4)
                    ratt[begin : begin + CHUNK, at : at + 128] = (got[:, :128] / got[:, 128:]).astype(BF16)
        mixed = mm(ratt[...], rproj[...])
        low, high = layer_norm(low.astype(F32) + mixed[:, 0:128], high + mixed[:, 128:256])
        done[f, :, 0:32, :] = low.astype(BF16).reshape(PEERS, 32, 128)
        high = high.reshape(PEERS, 2, 16, 128)
        high = high[:, 0] + pltpu.roll(high[:, 1].reshape(PEERS * 16, 128), 64, 1).reshape(PEERS, 16, 128)
        done[f, :, 32:48, :] = high.astype(BF16)

        def to_peer(k, _):
            p = lax.rem(me + k, PEERS)
            pass_on(
                done.at[f, p],
                normed.at[f, place(p)],
                k,
                "cells",
                p,
                send2_sem,
                recv2_sem.at[f],
            )
            return 0

        return lax.fori_loop(0, PEERS, to_peer, 0)

    lax.fori_loop(0, OWN, column, 0)

    def unpack(f, _):
        pltpu.make_async_copy(normed.at[f], normed.at[f], recv2_sem.at[f]).wait()
        for p in range(PEERS):
            at = pl.multiple_of((p * OWN + f) * STRIDE, 8)
            turn0[pl.ds(at, LOCAL), :] = normed[f, p, 0:32, :].astype(F32)
            high = normed[f, p, 32:48, :].astype(F32)
            turn1[pl.ds(at, 16), :] = high
            turn1[pl.ds(at + 16, 16), :] = pltpu.roll(high, 64, 1)
        return 0

    all_cot.wait()
    lax.fori_loop(0, OWN, unpack, 0)

    def feed(step, _):
        feed_forward(BLOCKS * step, cot_ref, turn0, turn1, win_t, wout, toks, acts, dcot, sums)
        return 0

    lax.fori_loop(0, STEPS // BLOCKS, feed, 0)

    def output(step, _):
        output_cells(step, wout_t, toks, acts, out_ref)
        return 0

    factor = 1.0 / math.sqrt(16 * ROWS * FEATS)
    part[0] = (sums[0, :, 0:128] * factor).astype(BF16)
    part[1] = (sums[1, :, 0:128] * (0.5 * factor)).astype(BF16)
    part[2, :, 0:64] = (sums[0, :, 128:192] * factor).astype(BF16)
    part[2, :, 64:128] = (sums[1, :, 128:192] * (0.5 * factor)).astype(BF16)

    table = lax.axis_index("tables") if remote else 0
    chip = me // 2
    core = me - 2 * chip
    theirs = pl.ds(pl.multiple_of((1 - core) * 384, 384), 384)
    mine = pl.ds(pl.multiple_of(core * 384, 384), 384)
    if remote:
        swap = pltpu.make_async_remote_copy(
            src_ref=part.at[:, theirs, :],
            dst_ref=pair,
            send_sem=sums_sem.at[0],
            recv_sem=sums_sem.at[1],
            device_id={"cells": 2 * chip + 1 - core},
            device_id_type=MESH,
        )
    else:
        swap = pltpu.make_async_copy(part.at[:, theirs, :], pair, sums_sem.at[1])
    swap.start()
    lax.fori_loop(0, STEPS // 8, output, 0)
    swap.wait()
    for t in range(3):
        half_sum[t] = (part[t, mine, :].astype(F32) + pair[t].astype(F32)).astype(BF16)

    def to_chip(k, _):
        p = lax.rem(chip + k, CHIPS)
        source = half_sum.at[:, pl.ds(pl.multiple_of(48 * p, 16), 48), :]
        target = got_chips.at[chip if remote else p]
        pass_on(source, target, k, "cells", 2 * p + core, sums_sem.at[2], sums_sem.at[3])
        return 0

    lax.fori_loop(0, CHIPS, to_chip, 0)
    lined[...] = jnp.zeros(lined.shape, F32)
    lax.fori_loop(STEPS // 8, STEPS * 5 // 8, output, 0)
    pltpu.make_async_copy(got_chips, got_chips, sums_sem.at[3]).wait()
    total = got_chips[0].astype(F32)
    for p in range(1, CHIPS):
        total = total + got_chips[p].astype(F32)
    for t in range(PEERS):
        for i in range(3):
            lined[t, 4 * i : 4 * i + 3, :] = total[i, 3 * t : 3 * t + 3, :]
    row[...] = lined[...].astype(BF16)

    def to_table(k, _):
        p = lax.rem(table + k, PEERS)
        pass_on(row.at[p], got_tables.at[table if remote else p], k, "tables", p, sums_sem.at[4], sums_sem.at[5])
        return 0

    lax.fori_loop(0, PEERS, to_table, 0)
    lax.fori_loop(STEPS * 5 // 8, STEPS, output, 0)
    if remote:
        sent = send.at[pl.ds(0, PEERS - 1)]
        pltpu.make_async_copy(sent, sent, send_sem).wait()
        sent = normed.at[:, pl.ds(0, PEERS - 1)]
        pltpu.make_async_copy(sent, sent, send2_sem).wait()
        sent = got_chips.at[pl.ds(0, CHIPS - 1)]
        pltpu.make_async_copy(sent, sent, sums_sem.at[2]).wait()
        sent = got_tables.at[pl.ds(0, PEERS - 1)]
        pltpu.make_async_copy(sent, sent, sums_sem.at[4]).wait()
    pltpu.make_async_copy(got_tables, got_tables, sums_sem.at[5]).wait()
    final = got_tables[0].astype(F32)
    for t in range(1, PEERS):
        final = final + got_tables[t].astype(F32)
    grad_in_ref[:, 0:128] = final[0:3, :]
    grad_in_ref[:, 128:192] = final[8:11, 0:64]
    grad_out_ref[:, 0:128] = final[4:7, :]
    grad_out_ref[:, 128:192] = final[8:11, 64:128]


def whole_layer(
    x_t, feat_count, train_count, feat_qkv, feat_proj, row_qkv, row_proj, w_in, w_out_t, cot_t, remote=True
):
    vmem = pl.BlockSpec(memory_space=pltpu.VMEM)
    smem = pl.BlockSpec(memory_space=pltpu.SMEM)
    hbm = pl.BlockSpec(memory_space=pltpu.HBM)
    return pl.pallas_call(
        functools.partial(layer_kernel, remote),
        name="layer",
        out_shape=(
            jax.ShapeDtypeStruct((LOCAL, E, FEATS), BF16),
            jax.ShapeDtypeStruct((3, E), F32),
            jax.ShapeDtypeStruct((3, E), F32),
        ),
        in_specs=[smem, smem, hbm] + [vmem] * 6 + [hbm],
        out_specs=(vmem, vmem, vmem),
        scratch_shapes=[
            pltpu.VMEM((256, 768), BF16),
            pltpu.VMEM((256, 256), BF16),
            pltpu.VMEM((256, 768), BF16),
            pltpu.VMEM((256, 256), BF16),
            pltpu.VMEM((FBLOCK * FEATS, 256), F32),
            pltpu.VMEM((FBLOCK * FEATS, 256), F32),
            pltpu.VMEM((FBLOCK * FEATS, 768), F32),
            pltpu.VMEM((FBLOCK, 512, 256), BF16),
            pltpu.VMEM((FBLOCK, 256, 256), BF16),
            pltpu.VMEM((FBLOCK * FEATS, 256), BF16),
            pltpu.VMEM((FEATS * STRIDE, 128), F32),
            pltpu.VMEM((FEATS * STRIDE, 128), F32),
            pltpu.VMEM((PEERS, 2, TILES, 16, 128), BF16),
            pltpu.VMEM((2, PEERS, TILES, 16, 128), BF16),
            pltpu.VMEM((ROWS, 256), BF16),
            pltpu.VMEM((KEYS, 512), BF16),
            pltpu.VMEM((HEADS * KEYS, 128), BF16),
            pltpu.VMEM((HEADS * KEYS, 256), BF16),
            pltpu.VMEM((ROWS, 256), BF16),
            pltpu.VMEM((OWN, PEERS, 48, 128), BF16),
            pltpu.VMEM((LOCAL, E, FEATS), BF16),
            pltpu.VMEM((LOCAL, E, FEATS), BF16),
            pltpu.VMEM((OWN, PEERS, 48, 128), BF16),
            pltpu.VMEM((HID, E), BF16),
            pltpu.VMEM((HID, E), BF16),
            pltpu.VMEM((E, HID), BF16),
            pltpu.VMEM((STEPS, DTOK, E), BF16),
            pltpu.VMEM((STEPS, HID, DTOK), BF16),
            pltpu.VMEM((BLOCKS, E, DTOK), BF16),
            pltpu.VMEM((2, HID, E), F32),
            pltpu.VMEM((3, HID, 128), BF16),
            pltpu.VMEM((3, 384, 128), BF16),
            pltpu.VMEM((3, 384, 128), BF16),
            pltpu.VMEM((CHIPS, 3, 48, 128), BF16),
            pltpu.VMEM((PEERS, 16, 128), F32),
            pltpu.VMEM((PEERS, 16, 128), BF16),
            pltpu.VMEM((PEERS, 16, 128), BF16),
            pltpu.SemaphoreType.DMA,
            pltpu.SemaphoreType.DMA((5,)),
            pltpu.SemaphoreType.DMA,
            pltpu.SemaphoreType.DMA((OWN,)),
            pltpu.SemaphoreType.DMA((3,)),
            pltpu.SemaphoreType.DMA((6,)),
        ],
        compiler_params=pltpu.CompilerParams(
            collective_id=0 if remote else None, has_side_effects=True, vmem_limit_bytes=VMEM_LIMIT
        ),
    )(feat_count, train_count, x_t, feat_qkv, feat_proj, row_qkv, row_proj, w_in, w_out_t, cot_t)


def per_device(
    cells_in, train_count, feat_count, feat_qkv, feat_proj, row_qkv, row_proj, w_in, w_out, cotangent
):
    x_t = jnp.swapaxes(cells_in[0], 1, 2)
    cot_t = jnp.swapaxes(cotangent[0], 1, 2)
    out_t, grad_in, grad_out = whole_layer(
        x_t, feat_count, train_count, feat_qkv, feat_proj, row_qkv, row_proj, w_in, w_out.T, cot_t
    )
    return (jnp.swapaxes(out_t, 1, 2)[None], grad_in.T, grad_out)


def solution(mesh):
    return jax.shard_map(
        per_device,
        mesh=mesh,
        in_specs=(
            P("tables", "cells", None, None),
            P("tables"),
            P("tables"),
            P(),
            P(),
            P(),
            P(),
            P(),
            P(),
            P("tables", "cells", None, None),
        ),
        out_specs=(
            P("tables", "cells", None, None),
            P(None, ("tables", "cells")),
            P(("tables", "cells"), None),
        ),
        check_vma=False,
    )
```

```python
import functools
import math

import jax
import jax.numpy as jnp
from jax import lax
from jax.experimental import pallas as pl
from jax.experimental.pallas import tpu as pltpu
from jax.sharding import PartitionSpec as P

HEADS = 6
HEAD_DIM = 32
E = 192
HID = 768
FEATS = 112
ROWS = 512
LOCAL = 32
PEERS = 16
OWN = 7
KEYS = 384
STRIDE = 40
F32 = jnp.float32
BF16 = jnp.bfloat16
NEG = -1e30
QSCALE = math.log2(math.e) / math.sqrt(HEAD_DIM)
VMEM_LIMIT = 60 * 1024 * 1024
MESH = pl.DeviceIdType.MESH

NN = (((1,), (0,)), ((), ()))
NT = (((1,), (1,)), ((), ()))


def mm(a, b, dims=NN):
    return lax.dot_general(a, b, dims, preferred_element_type=F32)


def eye(n):
    r = lax.broadcasted_iota(jnp.int32, (n, n), 0)
    c = lax.broadcasted_iota(jnp.int32, (n, n), 1)
    return (r == c).astype(F32).astype(BF16)


def head_mask(head):
    lane = lax.broadcasted_iota(jnp.int32, (1, 128), 1)
    low = 32 * (head % 4)
    return ((lane >= low) & (lane < low + 32)).astype(F32).astype(BF16)


def ones_mask(head):
    lane = lax.broadcasted_iota(jnp.int32, (1, 128), 1)
    low = 32 * (head % 4)
    high = 128 if head == 5 else low + 32
    return ((lane >= low) & (lane < high)).astype(F32).astype(BF16)


def spread_weights(w_ref, wide_ref, proj_ref, proj_wide):
    wide_ref[...] = jnp.zeros(wide_ref.shape, BF16)
    for part in range(3):
        wide_ref[0:192, 256 * part : 256 * part + 192] = w_ref[:, 192 * part : 192 * part + 192]
    proj_wide[...] = jnp.zeros(proj_wide.shape, BF16)
    proj_wide[0:192, 0:192] = proj_ref[...]


def layer_norm(low, high):
    mean = (jnp.sum(low, axis=-1, keepdims=True) + jnp.sum(high, axis=-1, keepdims=True)) * (1.0 / E)
    low = low - mean
    half = lax.broadcasted_iota(jnp.int32, (1, 128), 1) < 64
    high = jnp.where(half, high - mean, 0.0)
    var = jnp.sum(low * low + high * high, axis=-1, keepdims=True) * (1.0 / E)
    scale = lax.rsqrt(var + 1e-05)
    return low * scale, high * scale


def greet(axes):
    barrier = pltpu.get_barrier_semaphore()
    for axis in axes:
        me = lax.axis_index(axis)

        @pl.loop(1, PEERS)
        def _(k):
            pl.semaphore_signal(
                barrier, inc=1, device_id={axis: lax.rem(me + k, PEERS)}, device_id_type=MESH
            )


def await_peers(axes):
    pl.semaphore_wait(pltpu.get_barrier_semaphore(), (PEERS - 1) * len(axes))


DROWS = 4
DTOK = DROWS * 128
HBLOCK = 256
BLOCKS = 2
AHEAD = 1
STEPS = LOCAL // DROWS
CHIPS = PEERS // 2


def order_hidden(win_ref, wout_ref, win_t, wout, wout_t):
    new = lax.broadcasted_iota(jnp.int32, (HID, 1), 0)
    old = lax.broadcasted_iota(jnp.int32, (HID, HID), 1)
    core = new // 384
    chip = (new - core * 384) // 48
    within = new - core * 384 - chip * 48
    table = within // 3
    place = table * 48 + (2 * chip + core) * 3 + (within - table * 3)
    perm = (old == place).astype(F32).astype(BF16)
    win_t[...] = mm(perm, win_ref[...], NT).astype(BF16)
    wout[...] = (0.5 * mm(perm, wout_ref[...], NT)).astype(BF16)
    wout_t[...] = (0.5 * mm(wout_ref[...], perm, NT)).astype(BF16)


def feed_forward(first, cot_ref, turn0, turn1, win_t, wout, toks, acts, cot, sums):
    units = []
    for b in range(BLOCKS):
        for j in range(DROWS):
            at = (first + b) * DROWS + j
            rows = pl.ds(128 * j, FEATS)
            toks[first + b, rows, 0:128] = turn0[pl.ds(at, FEATS, stride=STRIDE), :].astype(BF16)
            toks[first + b, rows, 128:192] = turn1[pl.ds(at, FEATS, stride=STRIDE), 0:64].astype(BF16)
            cot[b, :, 128 * j : 128 * j + FEATS] = cot_ref[at]
        units += [(b, begin) for begin in range(0, HID, HBLOCK)]
    waiting = []
    for n in range(len(units) + AHEAD):
        if n < len(units):
            b, begin = units[n]
            rows = pl.ds(begin, HBLOCK)
            waiting.append((mm(win_t[rows, :], toks[first + b], NT), mm(wout[rows, :], cot[b])))
        if n >= AHEAD:
            b, begin = units[n - AHEAD]
            rows = pl.ds(begin, HBLOCK)
            pre, dact = waiting.pop(0)
            u = pre * math.sqrt(0.5)
            twice = lax.erf(u) + 1.0
            act = (pre * twice).astype(BF16)
            slope = twice + u * jnp.exp2(math.log2(2.0 / math.sqrt(math.pi)) - (u * u) * math.log2(math.e))
            dpre = (dact * slope).astype(BF16)
            acts[first + b, rows, :] = act
            sums[0, rows, :] += mm(dpre, toks[first + b])
            sums[1, rows, :] += mm(act, cot[b], NT)


def output_cells(step, wout_t, toks, acts, out_ref):
    total = mm(eye(E), toks[step], NT) + mm(wout_t[...], acts[step])
    for j in range(DROWS):
        out_ref[step * DROWS + j] = total[:, 128 * j : 128 * j + FEATS].astype(BF16)


FBLOCK = 4
TILES = 11
CHUNK = 256
LAG = 2
FILL = 2


def layer_kernel(
    remote,
    feat_count,
    train_count,
    x_hbm,
    fw_hbm,
    fproj_hbm,
    rw_hbm,
    rproj_hbm,
    win_hbm,
    wout_hbm,
    cot_hbm,
    out_hbm,
    grad_in_ref,
    grad_out_ref,
    fwide,
    fproj,
    rwide,
    rproj,
    tok,
    kept,
    qkv,
    vals0,
    vals1,
    att,
    turn0,
    turn1,
    send,
    cols,
    rq,
    keys,
    vals,
    ratt,
    done,
    fw_ref,
    fproj_ref,
    rw_ref,
    rproj_ref,
    win_ref,
    wout_ref,
    x_ref,
    cot_ref,
    normed,
    win_t,
    wout,
    wout_t,
    toks,
    acts,
    dcot,
    sums,
    out_buf,
    part,
    pair,
    half_sum,
    got_chips,
    lined,
    row,
    got_tables,
    send_sem,
    cols_sem,
    send2_sem,
    recv2_sem,
    local_sem,
    sums_sem,
):
    me = lax.axis_index("cells") if remote else 0
    first_x = pltpu.make_async_copy(x_hbm.at[0:8], x_ref.at[0:8], local_sem.at[0])
    rest_x = pltpu.make_async_copy(x_hbm.at[8:LOCAL], x_ref.at[8:LOCAL], local_sem.at[1])
    all_cot = pltpu.make_async_copy(cot_hbm, cot_ref, local_sem.at[2])
    pairs = (
        (fw_hbm, fw_ref),
        (fproj_hbm, fproj_ref),
        (rw_hbm, rw_ref),
        (rproj_hbm, rproj_ref),
        (win_hbm, win_ref),
        (wout_hbm, wout_ref),
    )
    weights = [pltpu.make_async_copy(a, b, local_sem.at[4 + i]) for i, (a, b) in enumerate(pairs)]
    weights[0].start()
    weights[1].start()
    first_x.start()
    rest_x.start()
    for copy in weights[2:]:
        copy.start()
    all_cot.start()
    if remote:
        greet(("cells", "tables"))
    weights[0].wait()
    weights[1].wait()
    spread_weights(fw_ref, fwide, fproj_ref, fproj)
    ident = eye(FEATS)
    tok[:, 192:256] = jnp.zeros((FBLOCK * FEATS, 64), F32)
    lane = lax.broadcasted_iota(jnp.int32, (1, 128), 1)
    bias = jnp.where(lane < feat_count[0], 0.0, NEG).astype(F32)
    for ref, heads in ((vals0, range(4)), (vals1, range(4, 6))):
        ref[...] = jnp.zeros(ref.shape, BF16)
        for j in range(FBLOCK):
            for i, h in enumerate(heads):
                ref[j, 128 * i : 128 * i + FEATS, 128:256] = jnp.broadcast_to(ones_mask(h), (FEATS, 128))
    zero_pad = jnp.zeros((128 - FEATS, 128), BF16)

    def project(step):
        for j in range(FBLOCK):
            tok[pl.ds(FEATS * j, FEATS), 0:192] = mm(ident, x_ref[step * FBLOCK + j], NT)
        qkv[...] = mm(tok[...].astype(BF16), fwide[...])

    tiles_of_heads = ((range(4), vals0), (range(4, 6), vals1))

    def score_rows():
        scores = []
        for j in range(FBLOCK):
            rows = pl.ds(FEATS * j, FEATS)
            for tile, (heads, ref) in enumerate(tiles_of_heads):
                at = 128 * tile
                q = (qkv[rows, at : at + 128] * QSCALE).astype(BF16)
                k = qkv[rows, 256 + at : 384 + at].astype(BF16)
                v = qkv[rows, 512 + at : 640 + at].astype(BF16)
                pieces = []
                for i, h in enumerate(heads):
                    pieces += [k * head_mask(h), zero_pad]
                    ref[j, 128 * i : 128 * i + FEATS, 0:128] = v * head_mask(h)
                scores.append(mm(q, jnp.concatenate(pieces, axis=0), NT))
        return scores

    def attend(scores):
        for j in range(FBLOCK):
            rows = pl.ds(FEATS * j, FEATS)
            for tile, (heads, ref) in enumerate(tiles_of_heads):
                probs = []
                for i, h in enumerate(heads):
                    s = scores[2 * j + tile][:, 128 * i : 128 * i + 128] + bias
                    probs.append(jnp.exp2(s - jnp.max(s, axis=-1, keepdims=True)).astype(BF16))
                got = mm(jnp.concatenate(probs, axis=1), ref[j])
                att[rows, 128 * tile : 128 * tile + 128] = (got[:, :128] / got[:, 128:]).astype(BF16)

    def finish(step):
        mixed = mm(att[...], fproj[...])
        low, high = layer_norm(kept[:, 0:128] + mixed[:, 0:128], kept[:, 128:256] + mixed[:, 128:256])
        for j in range(FBLOCK):
            at = step * FBLOCK + j
            turn0[pl.ds(at, FEATS, stride=STRIDE), :] = low[FEATS * j : FEATS * j + FEATS]
            turn1[pl.ds(at, FEATS, stride=STRIDE), :] = high[FEATS * j : FEATS * j + FEATS]

    def blocks(step, _):
        scores = score_rows()
        finish(step - 2)
        kept[...] = tok[...]
        project(step)
        attend(scores)
        return 0

    def pack(p, group, half):
        def rows_of(ref, f):
            return ref[pl.ds(pl.multiple_of((p * OWN + f) * STRIDE + 16 * half, 8), 16), :]

        f = 2 * group
        at = 3 * group
        send[p, half, at] = rows_of(turn0, f).astype(BF16)
        high = rows_of(turn1, f)
        if f + 1 < OWN:
            at += 1
            send[p, half, at] = rows_of(turn0, f + 1).astype(BF16)
            high = high + pltpu.roll(rows_of(turn1, f + 1), 64, 1)
        send[p, half, at + 1] = high.astype(BF16)

    def pass_on(source, target, k, axis, p, send_s, recv_s):
        if not remote:
            pltpu.make_async_copy(source, target, recv_s).start()
            return

        @pl.when(k == 0)
        def _():
            pltpu.make_async_copy(source, target, recv_s).start()

        @pl.when(k != 0)
        def _():
            pltpu.make_async_remote_copy(
                src_ref=source,
                dst_ref=target,
                send_sem=send_s,
                recv_sem=recv_s,
                device_id={axis: p},
                device_id_type=MESH,
            ).start()

    def place(p):
        return me if remote else p

    first_x.wait()
    project(0)
    scores = score_rows()
    kept[...] = tok[...]
    project(1)
    attend(scores)
    rest_x.wait()
    lax.fori_loop(2, 2 + 16 // FBLOCK, blocks, 0)
    if remote:
        await_peers(("cells", "tables"))

    def first_half(k, _):
        p = lax.rem(me + k, PEERS)
        for group in range(4):
            pack(p, group, 0)
        pass_on(
            send.at[p, 0],
            cols.at[0, place(p)],
            k,
            "cells",
            p,
            send_sem,
            cols_sem.at[4],
        )
        return 0

    lax.fori_loop(0, PEERS, first_half, 0)
    lax.fori_loop(2 + 16 // FBLOCK, 32 // FBLOCK, blocks, 0)
    scores = score_rows()
    finish(32 // FBLOCK - 2)
    kept[...] = tok[...]
    attend(scores)
    finish(32 // FBLOCK - 1)
    for group in range(4):
        tiles = pl.ds(3 * group, min(3, TILES - 3 * group))

        def second_half(k, _):
            p = lax.rem(me + k, PEERS)
            pack(p, group, 1)
            pass_on(
                send.at[p, 1, tiles],
                cols.at[1, place(p), tiles],
                k,
                "cells",
                p,
                send_sem,
                cols_sem.at[group],
            )
            return 0

        lax.fori_loop(0, PEERS, second_half, 0)

    for copy in weights[2:]:
        copy.wait()
    spread_weights(rw_ref, rwide, rproj_ref, rproj)
    lane = lax.broadcasted_iota(jnp.int32, (1, KEYS), 1)
    rbias = jnp.where(lane < train_count[0], 0.0, NEG).astype(F32)
    for h in range(HEADS):
        for odd in range(2):
            vals[odd, KEYS * h : KEYS * h + KEYS, 128:256] = jnp.broadcast_to(ones_mask(h), (KEYS, 128))
    half_lane = lax.broadcasted_iota(jnp.int32, (1, 128), 1) < 64
    order_hidden(win_ref, wout_ref, win_t, wout, wout_t)
    sums[...] = jnp.zeros(sums.shape, F32)
    toks[...] = jnp.zeros(toks.shape, BF16)
    dcot[...] = jnp.zeros(dcot.shape, BF16)

    def arrive(f):
        for group in range(4):

            @pl.when(f == 2 * group)
            def _():
                ref = cols.at[1, :, pl.ds(3 * group, min(3, TILES - 3 * group))]
                pltpu.make_async_copy(ref, ref, cols_sem.at[group]).wait()

    def column_of(f, odd):
        at = 3 * (f // 2)

        def tokens(tile):
            return jnp.stack([cols[0, :, tile], cols[1, :, tile]], axis=1).reshape(ROWS, 128)

        low = tokens(at + odd)
        high = tokens(jnp.minimum(at + 2, TILES - 1)).astype(F32)
        if odd:
            high = pltpu.roll(high, 64, 1)
        return low, jnp.where(half_lane, high, 0.0)

    def prepare(f, odd):
        low, high = column_of(f, odd)
        x = jnp.concatenate([low, high.astype(BF16)], axis=1)
        rq[odd] = (mm(x, rwide[:, 0:256]) * QSCALE).astype(BF16)
        rkv = mm(x[0:KEYS], rwide[:, 256:768]).astype(BF16)
        for h in range(HEADS):
            at = 128 * (h // 4)
            rows = pl.ds(KEYS * h, KEYS)
            keys[odd, rows, :] = rkv[:, at : at + 128] * head_mask(h)
            vals[odd, rows, 0:128] = rkv[:, 256 + at : 384 + at] * head_mask(h)

    units = [(begin, first) for begin in range(0, ROWS, CHUNK) for first in (0, 2, 4)]

    def score_pair(odd, begin, first):
        at = 128 * (first // 4)
        return mm(rq[odd, begin : begin + CHUNK, at : at + 128], keys[odd, pl.ds(KEYS * first, 2 * KEYS), :], NT)

    def value_pair(odd, first, score):
        probs = []
        for i in range(2):
            s = score[:, KEYS * i : KEYS * i + KEYS] + rbias
            probs.append(jnp.exp2(s - jnp.max(s, axis=-1, keepdims=True)).astype(BF16))
        return mm(jnp.concatenate(probs, axis=1), vals[odd, pl.ds(KEYS * first, 2 * KEYS), :])

    def attend_rows(odd, fill=None):
        waiting = []
        got = None
        for n in range(len(units) + LAG):
            if n < len(units):
                waiting.append(score_pair(odd, *units[n]))
            if n == FILL and fill is not None:
                fill()
            if n >= LAG:
                begin, first = units[n - LAG]
                more = value_pair(odd, first, waiting.pop(0))
                got = more if first != 2 else got + more
                if first:
                    at = 128 * (first // 4)
                    ratt[odd, begin : begin + CHUNK, at : at + 128] = (got[:, :128] / got[:, 128:]).astype(BF16)

    def finish_column(f, odd):
        low, high = column_of(f, odd)
        mixed = mm(ratt[odd], rproj[...])
        low, high = layer_norm(low.astype(F32) + mixed[:, 0:128], high + mixed[:, 128:256])
        done[f, :, 0:32, :] = low.astype(BF16).reshape(PEERS, 32, 128)
        high = high.reshape(PEERS, 2, 16, 128)
        high = high[:, 0] + pltpu.roll(high[:, 1].reshape(PEERS * 16, 128), 64, 1).reshape(PEERS, 16, 128)
        done[f, :, 32:48, :] = high.astype(BF16)

    def send_column(f):
        def to_peer(k, _):
            p = lax.rem(me + k, PEERS)
            pass_on(done.at[f, p], normed.at[f, place(p)], k, "cells", p, send2_sem, recv2_sem.at[f])
            return 0

        lax.fori_loop(0, PEERS, to_peer, 0)

    pltpu.make_async_copy(cols.at[0], cols.at[0], cols_sem.at[4]).wait()
    arrive(0)
    prepare(0, 0)
    attend_rows(0, lambda: prepare(1, 1))

    def two_columns(g, _):
        f = 2 * g
        arrive(f)

        def fill():
            finish_column(f - 2, 0)
            prepare(f, 0)

        attend_rows(1, fill)
        send_column(f - 2)

        def fill_next():
            finish_column(f - 1, 1)

            prepare(jnp.minimum(f + 1, OWN - 2), 1)

        attend_rows(0, fill_next)
        send_column(f - 1)
        return 0

    lax.fori_loop(1, 4, two_columns, 0)
    finish_column(OWN - 1, 0)
    send_column(OWN - 1)

    def unpack(f, _):
        pltpu.make_async_copy(normed.at[f], normed.at[f], recv2_sem.at[f]).wait()
        for p in range(PEERS):
            at = pl.multiple_of((p * OWN + f) * STRIDE, 8)
            turn0[pl.ds(at, LOCAL), :] = normed[f, p, 0:32, :].astype(F32)
            high = normed[f, p, 32:48, :].astype(F32)
            turn1[pl.ds(at, 16), :] = high
            turn1[pl.ds(at + 16, 16), :] = pltpu.roll(high, 64, 1)
        return 0

    all_cot.wait()
    lax.fori_loop(0, OWN, unpack, 0)

    def feed(step, _):
        feed_forward(BLOCKS * step, cot_ref, turn0, turn1, win_t, wout, toks, acts, dcot, sums)
        return 0

    lax.fori_loop(0, STEPS // BLOCKS, feed, 0)

    def output(step, _):
        output_cells(step, wout_t, toks, acts, out_buf)
        rows = pl.ds(step * DROWS, DROWS)
        pltpu.make_async_copy(out_buf.at[rows], out_hbm.at[rows], local_sem.at[3]).start()
        return 0

    factor = 1.0 / math.sqrt(16 * ROWS * FEATS)
    part[0] = (sums[0, :, 0:128] * factor).astype(BF16)
    part[1] = (sums[1, :, 0:128] * (0.5 * factor)).astype(BF16)
    part[2, :, 0:64] = (sums[0, :, 128:192] * factor).astype(BF16)
    part[2, :, 64:128] = (sums[1, :, 128:192] * (0.5 * factor)).astype(BF16)

    table = lax.axis_index("tables") if remote else 0
    chip = me // 2
    core = me - 2 * chip
    theirs = pl.ds(pl.multiple_of((1 - core) * 384, 384), 384)
    mine = pl.ds(pl.multiple_of(core * 384, 384), 384)
    if remote:
        swap = pltpu.make_async_remote_copy(
            src_ref=part.at[:, theirs, :],
            dst_ref=pair,
            send_sem=sums_sem.at[0],
            recv_sem=sums_sem.at[1],
            device_id={"cells": 2 * chip + 1 - core},
            device_id_type=MESH,
        )
    else:
        swap = pltpu.make_async_copy(part.at[:, theirs, :], pair, sums_sem.at[1])
    swap.start()
    lax.fori_loop(0, STEPS // 8, output, 0)
    swap.wait()
    for t in range(3):
        half_sum[t] = (part[t, mine, :].astype(F32) + pair[t].astype(F32)).astype(BF16)

    def to_chip(k, _):
        p = lax.rem(chip + k, CHIPS)
        source = half_sum.at[:, pl.ds(pl.multiple_of(48 * p, 16), 48), :]
        target = got_chips.at[chip if remote else p]
        pass_on(source, target, k, "cells", 2 * p + core, sums_sem.at[2], sums_sem.at[3])
        return 0

    lax.fori_loop(0, CHIPS, to_chip, 0)
    lined[...] = jnp.zeros(lined.shape, F32)
    lax.fori_loop(STEPS // 8, STEPS * 5 // 8, output, 0)
    pltpu.make_async_copy(got_chips, got_chips, sums_sem.at[3]).wait()
    total = got_chips[0].astype(F32)
    for p in range(1, CHIPS):
        total = total + got_chips[p].astype(F32)
    for t in range(PEERS):
        for i in range(3):
            lined[t, 4 * i : 4 * i + 3, :] = total[i, 3 * t : 3 * t + 3, :]
    row[...] = lined[...].astype(BF16)

    def to_table(k, _):
        p = lax.rem(table + k, PEERS)
        pass_on(row.at[p], got_tables.at[table if remote else p], k, "tables", p, sums_sem.at[4], sums_sem.at[5])
        return 0

    lax.fori_loop(0, PEERS, to_table, 0)
    lax.fori_loop(STEPS * 5 // 8, STEPS, output, 0)
    if remote:
        sent = send.at[pl.ds(0, PEERS - 1)]
        pltpu.make_async_copy(sent, sent, send_sem).wait()
        sent = normed.at[:, pl.ds(0, PEERS - 1)]
        pltpu.make_async_copy(sent, sent, send2_sem).wait()
        sent = got_chips.at[pl.ds(0, CHIPS - 1)]
        pltpu.make_async_copy(sent, sent, sums_sem.at[2]).wait()
        sent = got_tables.at[pl.ds(0, PEERS - 1)]
        pltpu.make_async_copy(sent, sent, sums_sem.at[4]).wait()
    pltpu.make_async_copy(out_buf, out_hbm, local_sem.at[3]).wait()
    pltpu.make_async_copy(got_tables, got_tables, sums_sem.at[5]).wait()
    final = got_tables[0].astype(F32)
    for t in range(1, PEERS):
        final = final + got_tables[t].astype(F32)
    grad_in_ref[:, 0:128] = final[0:3, :]
    grad_in_ref[:, 128:192] = final[8:11, 0:64]
    grad_out_ref[:, 0:128] = final[4:7, :]
    grad_out_ref[:, 128:192] = final[8:11, 64:128]


def whole_layer(
    x_t, feat_count, train_count, feat_qkv, feat_proj, row_qkv, row_proj, w_in, w_out_t, cot_t, remote=True
):
    vmem = pl.BlockSpec(memory_space=pltpu.VMEM)
    smem = pl.BlockSpec(memory_space=pltpu.SMEM)
    hbm = pl.BlockSpec(memory_space=pl.ANY)
    return pl.pallas_call(
        functools.partial(layer_kernel, remote),
        name="layer",
        out_shape=(
            jax.ShapeDtypeStruct((LOCAL, E, FEATS), BF16),
            jax.ShapeDtypeStruct((3, E), F32),
            jax.ShapeDtypeStruct((3, E), F32),
        ),
        in_specs=[smem, smem] + [hbm] * 8,
        out_specs=(hbm, vmem, vmem),
        scratch_shapes=[
            pltpu.VMEM((256, 768), BF16),
            pltpu.VMEM((256, 256), BF16),
            pltpu.VMEM((256, 768), BF16),
            pltpu.VMEM((256, 256), BF16),
            pltpu.VMEM((FBLOCK * FEATS, 256), F32),
            pltpu.VMEM((FBLOCK * FEATS, 256), F32),
            pltpu.VMEM((FBLOCK * FEATS, 768), F32),
            pltpu.VMEM((FBLOCK, 512, 256), BF16),
            pltpu.VMEM((FBLOCK, 256, 256), BF16),
            pltpu.VMEM((FBLOCK * FEATS, 256), BF16),
            pltpu.VMEM((FEATS * STRIDE, 128), F32),
            pltpu.VMEM((FEATS * STRIDE, 128), F32),
            pltpu.VMEM((PEERS, 2, TILES, 16, 128), BF16),
            pltpu.VMEM((2, PEERS, TILES, 16, 128), BF16),
            pltpu.VMEM((2, ROWS, 256), BF16),
            pltpu.VMEM((2, HEADS * KEYS, 128), BF16),
            pltpu.VMEM((2, HEADS * KEYS, 256), BF16),
            pltpu.VMEM((2, ROWS, 256), BF16),
            pltpu.VMEM((OWN, PEERS, 48, 128), BF16),
            pltpu.VMEM((E, 3 * E), BF16),
            pltpu.VMEM((E, E), BF16),
            pltpu.VMEM((E, 3 * E), BF16),
            pltpu.VMEM((E, E), BF16),
            pltpu.VMEM((E, HID), BF16),
            pltpu.VMEM((E, HID), BF16),
            pltpu.VMEM((LOCAL, E, FEATS), BF16),
            pltpu.VMEM((LOCAL, E, FEATS), BF16),
            pltpu.VMEM((OWN, PEERS, 48, 128), BF16),
            pltpu.VMEM((HID, E), BF16),
            pltpu.VMEM((HID, E), BF16),
            pltpu.VMEM((E, HID), BF16),
            pltpu.VMEM((STEPS, DTOK, E), BF16),
            pltpu.VMEM((STEPS, HID, DTOK), BF16),
            pltpu.VMEM((BLOCKS, E, DTOK), BF16),
            pltpu.VMEM((2, HID, E), F32),
            pltpu.VMEM((LOCAL, E, FEATS), BF16),
            pltpu.VMEM((3, HID, 128), BF16),
            pltpu.VMEM((3, 384, 128), BF16),
            pltpu.VMEM((3, 384, 128), BF16),
            pltpu.VMEM((CHIPS, 3, 48, 128), BF16),
            pltpu.VMEM((PEERS, 16, 128), F32),
            pltpu.VMEM((PEERS, 16, 128), BF16),
            pltpu.VMEM((PEERS, 16, 128), BF16),
            pltpu.SemaphoreType.DMA,
            pltpu.SemaphoreType.DMA((5,)),
            pltpu.SemaphoreType.DMA,
            pltpu.SemaphoreType.DMA((OWN,)),
            pltpu.SemaphoreType.DMA((10,)),
            pltpu.SemaphoreType.DMA((6,)),
        ],
        compiler_params=pltpu.CompilerParams(
            collective_id=0 if remote else None, has_side_effects=True, vmem_limit_bytes=VMEM_LIMIT
        ),
    )(feat_count, train_count, x_t, feat_qkv, feat_proj, row_qkv, row_proj, w_in, w_out_t, cot_t)


PIECES = 8


def closing_kernel(cells_hbm, a_hbm, b_hbm, cells_out, a_out, b_out, cells, a, b, in_sem, out_sem):
    small = ((a_hbm, a, a_out), (b_hbm, b, b_out))
    size = LOCAL // PIECES
    steps = [(source, hold, target) for source, hold, target in small]
    steps += [tuple(ref.at[pl.ds(size * i, size)] for ref in (cells_hbm, cells, cells_out)) for i in range(PIECES)]
    loads = [pltpu.make_async_copy(source, hold, in_sem.at[i]) for i, (source, hold, _) in enumerate(steps)]
    stores = [pltpu.make_async_copy(hold, target, out_sem.at[i]) for i, (_, hold, target) in enumerate(steps)]
    for copy in loads:
        copy.start()
    for load, store in zip(loads, stores):
        load.wait()
        store.start()
    for copy in stores:
        copy.wait()


def close(cells, a, b):
    hbm = pl.BlockSpec(memory_space=pl.ANY)
    return pl.pallas_call(
        closing_kernel,
        name="closing_copies",
        out_shape=tuple(jax.ShapeDtypeStruct(v.shape, v.dtype) for v in (cells, a, b)),
        in_specs=[hbm] * 3,
        out_specs=(hbm,) * 3,
        scratch_shapes=[pltpu.VMEM(v.shape, v.dtype) for v in (cells, a, b)]
        + [pltpu.SemaphoreType.DMA((PIECES + 2,)), pltpu.SemaphoreType.DMA((PIECES + 2,))],
        compiler_params=pltpu.CompilerParams(vmem_limit_bytes=VMEM_LIMIT),
    )(cells, a, b)


def per_device(
    cells_in, train_count, feat_count, feat_qkv, feat_proj, row_qkv, row_proj, w_in, w_out, cotangent
):
    x_t = jnp.swapaxes(cells_in[0], 1, 2)
    cot_t = jnp.swapaxes(cotangent[0], 1, 2)
    out_t, grad_in, grad_out = whole_layer(
        x_t, feat_count, train_count, feat_qkv, feat_proj, row_qkv, row_proj, w_in, w_out.T, cot_t
    )
    out_t, grad_in, grad_out = close(out_t, grad_in, grad_out)
    return (jnp.swapaxes(out_t, 1, 2)[None], grad_in.T, grad_out)


def solution(mesh):
    return jax.shard_map(
        per_device,
        mesh=mesh,
        in_specs=(
            P("tables", "cells", None, None),
            P("tables"),
            P("tables"),
            P(),
            P(),
            P(),
            P(),
            P(),
            P(),
            P("tables", "cells", None, None),
        ),
        out_specs=(
            P("tables", "cells", None, None),
            P(None, ("tables", "cells")),
            P(("tables", "cells"), None),
        ),
        check_vma=False,
    )
```

```python
import functools
import math

import jax
import jax.numpy as jnp
from jax import lax
from jax.experimental import pallas as pl
from jax.experimental.pallas import tpu as pltpu
from jax.sharding import PartitionSpec as P

HEADS = 6
HEAD_DIM = 32
E = 192
HID = 768
FEATS = 112
ROWS = 512
LOCAL = 32
PEERS = 16
OWN = 7
KEYS = 384
STRIDE = 40
F32 = jnp.float32
BF16 = jnp.bfloat16
NEG = -1e30
QSCALE = math.log2(math.e) / math.sqrt(HEAD_DIM)
VMEM_LIMIT = 60 * 1024 * 1024
MESH = pl.DeviceIdType.MESH

NN = (((1,), (0,)), ((), ()))
NT = (((1,), (1,)), ((), ()))


def mm(a, b, dims=NN):
    return lax.dot_general(a, b, dims, preferred_element_type=F32)


def eye(n):
    r = lax.broadcasted_iota(jnp.int32, (n, n), 0)
    c = lax.broadcasted_iota(jnp.int32, (n, n), 1)
    return (r == c).astype(F32).astype(BF16)


def head_mask(head):
    lane = lax.broadcasted_iota(jnp.int32, (1, 128), 1)
    low = 32 * (head % 4)
    return ((lane >= low) & (lane < low + 32)).astype(F32).astype(BF16)


def ones_mask(head):
    lane = lax.broadcasted_iota(jnp.int32, (1, 128), 1)
    low = 32 * (head % 4)
    high = 128 if head == 5 else low + 32
    return ((lane >= low) & (lane < high)).astype(F32).astype(BF16)


def spread_weights(w_ref, wide_ref, proj_ref, proj_wide):
    wide_ref[...] = jnp.zeros(wide_ref.shape, BF16)
    for part in range(3):
        wide_ref[0:192, 256 * part : 256 * part + 192] = w_ref[:, 192 * part : 192 * part + 192]
    proj_wide[...] = jnp.zeros(proj_wide.shape, BF16)
    proj_wide[0:192, 0:192] = proj_ref[...]


def layer_norm(low, high):
    mean = (jnp.sum(low, axis=-1, keepdims=True) + jnp.sum(high, axis=-1, keepdims=True)) * (1.0 / E)
    low = low - mean
    half = lax.broadcasted_iota(jnp.int32, (1, 128), 1) < 64
    high = jnp.where(half, high - mean, 0.0)
    var = jnp.sum(low * low + high * high, axis=-1, keepdims=True) * (1.0 / E)
    scale = lax.rsqrt(var + 1e-05)
    return low * scale, high * scale


def greet(axes):
    barrier = pltpu.get_barrier_semaphore()
    for axis in axes:
        me = lax.axis_index(axis)

        @pl.loop(1, PEERS)
        def _(k):
            pl.semaphore_signal(
                barrier, inc=1, device_id={axis: lax.rem(me + k, PEERS)}, device_id_type=MESH
            )


def await_peers(axes):
    pl.semaphore_wait(pltpu.get_barrier_semaphore(), (PEERS - 1) * len(axes))


DROWS = 4
DTOK = DROWS * 128
HBLOCK = 256
BLOCKS = 2
AHEAD = 2
STEPS = LOCAL // DROWS
CHIPS = PEERS // 2


def order_hidden(win_ref, wout_ref, win_t, wout, wout_t):
    new = lax.broadcasted_iota(jnp.int32, (HID, 1), 0)
    old = lax.broadcasted_iota(jnp.int32, (HID, HID), 1)
    core = new // 384
    chip = (new - core * 384) // 48
    within = new - core * 384 - chip * 48
    table = within // 3
    place = table * 48 + (2 * chip + core) * 3 + (within - table * 3)
    perm = (old == place).astype(F32).astype(BF16)
    win_t[...] = mm(perm, win_ref[...], NT).astype(BF16)
    wout[...] = (0.5 * mm(perm, wout_ref[...], NT)).astype(BF16)
    wout_t[...] = (0.5 * mm(wout_ref[...], perm, NT)).astype(BF16)


def feed_forward(first, cot_ref, turn0, turn1, win_t, wout, toks, acts, cot, sums):
    units = []
    for b in range(BLOCKS):
        for j in range(DROWS):
            at = (first + b) * DROWS + j
            rows = pl.ds(128 * j, FEATS)
            toks[first + b, rows, 0:128] = turn0[pl.ds(at, FEATS, stride=STRIDE), :].astype(BF16)
            toks[first + b, rows, 128:192] = turn1[pl.ds(at, FEATS, stride=STRIDE), 0:64].astype(BF16)
            cot[b, :, 128 * j : 128 * j + FEATS] = cot_ref[at]
        units += [(b, begin) for begin in range(0, HID, HBLOCK)]
    waiting = []
    for n in range(len(units) + AHEAD):
        if n < len(units):
            b, begin = units[n]
            rows = pl.ds(begin, HBLOCK)
            waiting.append((mm(win_t[rows, :], toks[first + b], NT), mm(wout[rows, :], cot[b])))
        if n >= AHEAD:
            b, begin = units[n - AHEAD]
            rows = pl.ds(begin, HBLOCK)
            pre, dact = waiting.pop(0)
            u = pre * math.sqrt(0.5)
            twice = lax.erf(u) + 1.0
            act = (pre * twice).astype(BF16)
            slope = twice + u * jnp.exp2(math.log2(2.0 / math.sqrt(math.pi)) - (u * u) * math.log2(math.e))
            dpre = (dact * slope).astype(BF16)
            acts[first + b, rows, :] = act
            sums[0, rows, :] += mm(dpre, toks[first + b])
            sums[1, rows, :] += mm(act, cot[b], NT)


def output_cells(step, wout_t, toks, acts, out_ref):
    total = mm(eye(E), toks[step], NT) + mm(wout_t[...], acts[step])
    for j in range(DROWS):
        out_ref[step * DROWS + j] = total[:, 128 * j : 128 * j + FEATS].astype(BF16)


FBLOCK = 4
TILES = 11
CHUNK = 256
LAG = 2
FILL = 2


def layer_kernel(
    remote,
    feat_count,
    train_count,
    x_hbm,
    fw_hbm,
    fproj_hbm,
    rw_hbm,
    rproj_hbm,
    win_hbm,
    wout_hbm,
    cot_hbm,
    out_hbm,
    grad_in_ref,
    grad_out_ref,
    fwide,
    fproj,
    rwide,
    rproj,
    tok,
    kept,
    qkv,
    vals0,
    vals1,
    att,
    turn0,
    turn1,
    send,
    cols,
    rq,
    keys,
    vals,
    ratt,
    done,
    fw_ref,
    fproj_ref,
    rw_ref,
    rproj_ref,
    win_ref,
    wout_ref,
    x_ref,
    cot_ref,
    normed,
    win_t,
    wout,
    wout_t,
    toks,
    acts,
    dcot,
    sums,
    out_buf,
    part,
    pair,
    half_sum,
    got_chips,
    lined,
    row,
    got_tables,
    send_sem,
    cols_sem,
    send2_sem,
    recv2_sem,
    local_sem,
    sums_sem,
):
    me = lax.axis_index("cells") if remote else 0
    first_x = pltpu.make_async_copy(x_hbm.at[0:8], x_ref.at[0:8], local_sem.at[0])
    rest_x = pltpu.make_async_copy(x_hbm.at[8:LOCAL], x_ref.at[8:LOCAL], local_sem.at[1])
    all_cot = pltpu.make_async_copy(cot_hbm, cot_ref, local_sem.at[2])
    pairs = (
        (fw_hbm, fw_ref),
        (fproj_hbm, fproj_ref),
        (rw_hbm, rw_ref),
        (rproj_hbm, rproj_ref),
        (win_hbm, win_ref),
        (wout_hbm, wout_ref),
    )
    weights = [pltpu.make_async_copy(a, b, local_sem.at[4 + i]) for i, (a, b) in enumerate(pairs)]
    weights[0].start()
    weights[1].start()
    first_x.start()
    rest_x.start()
    for copy in weights[2:]:
        copy.start()
    all_cot.start()
    if remote:
        greet(("cells", "tables"))
    weights[0].wait()
    weights[1].wait()
    spread_weights(fw_ref, fwide, fproj_ref, fproj)
    ident = eye(FEATS)
    tok[:, 192:256] = jnp.zeros((FBLOCK * FEATS, 64), F32)
    lane = lax.broadcasted_iota(jnp.int32, (1, 128), 1)
    bias = jnp.where(lane < feat_count[0], 0.0, NEG).astype(F32)
    for ref, heads in ((vals0, range(4)), (vals1, range(4, 6))):
        ref[...] = jnp.zeros(ref.shape, BF16)
        for j in range(FBLOCK):
            for i, h in enumerate(heads):
                ref[j, 128 * i : 128 * i + FEATS, 128:256] = jnp.broadcast_to(ones_mask(h), (FEATS, 128))
    zero_pad = jnp.zeros((128 - FEATS, 128), BF16)

    def project(step):
        for j in range(FBLOCK):
            tok[pl.ds(FEATS * j, FEATS), 0:192] = mm(ident, x_ref[step * FBLOCK + j], NT)
        qkv[...] = mm(tok[...].astype(BF16), fwide[...])

    tiles_of_heads = ((range(4), vals0), (range(4, 6), vals1))

    def score_rows():
        scores = []
        for j in range(FBLOCK):
            rows = pl.ds(FEATS * j, FEATS)
            for tile, (heads, ref) in enumerate(tiles_of_heads):
                at = 128 * tile
                q = (qkv[rows, at : at + 128] * QSCALE).astype(BF16)
                k = qkv[rows, 256 + at : 384 + at].astype(BF16)
                v = qkv[rows, 512 + at : 640 + at].astype(BF16)
                pieces = []
                for i, h in enumerate(heads):
                    pieces += [k * head_mask(h), zero_pad]
                    ref[j, 128 * i : 128 * i + FEATS, 0:128] = v * head_mask(h)
                scores.append(mm(q, jnp.concatenate(pieces, axis=0), NT))
        return scores

    def attend(scores):
        for j in range(FBLOCK):
            rows = pl.ds(FEATS * j, FEATS)
            for tile, (heads, ref) in enumerate(tiles_of_heads):
                probs = []
                for i, h in enumerate(heads):
                    s = scores[2 * j + tile][:, 128 * i : 128 * i + 128] + bias
                    probs.append(jnp.exp2(s - jnp.max(s, axis=-1, keepdims=True)).astype(BF16))
                got = mm(jnp.concatenate(probs, axis=1), ref[j])
                att[rows, 128 * tile : 128 * tile + 128] = (got[:, :128] / got[:, 128:]).astype(BF16)

    def finish(step):
        mixed = mm(att[...], fproj[...])
        low, high = layer_norm(kept[:, 0:128] + mixed[:, 0:128], kept[:, 128:256] + mixed[:, 128:256])
        for j in range(FBLOCK):
            at = step * FBLOCK + j
            turn0[pl.ds(at, FEATS, stride=STRIDE), :] = low[FEATS * j : FEATS * j + FEATS]
            turn1[pl.ds(at, FEATS, stride=STRIDE), :] = high[FEATS * j : FEATS * j + FEATS]

    def blocks(step, _):
        scores = score_rows()
        finish(step - 2)
        kept[...] = tok[...]
        project(step)
        attend(scores)
        return 0

    def pack(p, group, half):
        def rows_of(ref, f):
            return ref[pl.ds(pl.multiple_of((p * OWN + f) * STRIDE + 16 * half, 8), 16), :]

        f = 2 * group
        at = 3 * group
        send[p, half, at] = rows_of(turn0, f).astype(BF16)
        high = rows_of(turn1, f)
        if f + 1 < OWN:
            at += 1
            send[p, half, at] = rows_of(turn0, f + 1).astype(BF16)
            high = high + pltpu.roll(rows_of(turn1, f + 1), 64, 1)
        send[p, half, at + 1] = high.astype(BF16)

    def pass_on(source, target, k, axis, p, send_s, recv_s):
        if not remote:
            pltpu.make_async_copy(source, target, recv_s).start()
            return

        @pl.when(k == 0)
        def _():
            pltpu.make_async_copy(source, target, recv_s).start()

        @pl.when(k != 0)
        def _():
            pltpu.make_async_remote_copy(
                src_ref=source,
                dst_ref=target,
                send_sem=send_s,
                recv_sem=recv_s,
                device_id={axis: p},
                device_id_type=MESH,
            ).start()

    def place(p):
        return me if remote else p

    first_x.wait()
    project(0)
    scores = score_rows()
    kept[...] = tok[...]
    project(1)
    attend(scores)
    rest_x.wait()
    lax.fori_loop(2, 2 + 16 // FBLOCK, blocks, 0)
    if remote:
        await_peers(("cells", "tables"))

    def first_half(k, _):
        p = lax.rem(me + k, PEERS)
        for group in range(4):
            pack(p, group, 0)
        pass_on(
            send.at[p, 0],
            cols.at[0, place(p)],
            k,
            "cells",
            p,
            send_sem,
            cols_sem.at[4],
        )
        return 0

    lax.fori_loop(0, PEERS, first_half, 0)
    lax.fori_loop(2 + 16 // FBLOCK, 32 // FBLOCK, blocks, 0)
    scores = score_rows()
    finish(32 // FBLOCK - 2)
    kept[...] = tok[...]
    attend(scores)
    finish(32 // FBLOCK - 1)
    for group in range(4):
        tiles = pl.ds(3 * group, min(3, TILES - 3 * group))

        def second_half(k, _):
            p = lax.rem(me + k, PEERS)
            pack(p, group, 1)
            pass_on(
                send.at[p, 1, tiles],
                cols.at[1, place(p), tiles],
                k,
                "cells",
                p,
                send_sem,
                cols_sem.at[group],
            )
            return 0

        lax.fori_loop(0, PEERS, second_half, 0)

    for copy in weights[2:]:
        copy.wait()
    spread_weights(rw_ref, rwide, rproj_ref, rproj)
    lane = lax.broadcasted_iota(jnp.int32, (1, KEYS), 1)
    rbias = jnp.where(lane < train_count[0], 0.0, NEG).astype(F32)
    for h in range(HEADS):
        for odd in range(2):
            vals[odd, KEYS * h : KEYS * h + KEYS, 128:256] = jnp.broadcast_to(ones_mask(h), (KEYS, 128))
    half_lane = lax.broadcasted_iota(jnp.int32, (1, 128), 1) < 64
    order_hidden(win_ref, wout_ref, win_t, wout, wout_t)
    sums[...] = jnp.zeros(sums.shape, F32)
    toks[...] = jnp.zeros(toks.shape, BF16)
    dcot[...] = jnp.zeros(dcot.shape, BF16)

    def arrive(f):
        for group in range(4):

            @pl.when(f == 2 * group)
            def _():
                ref = cols.at[1, :, pl.ds(3 * group, min(3, TILES - 3 * group))]
                pltpu.make_async_copy(ref, ref, cols_sem.at[group]).wait()

    def column_of(f, odd):
        at = 3 * (f // 2)

        def tokens(tile):
            return jnp.stack([cols[0, :, tile], cols[1, :, tile]], axis=1).reshape(ROWS, 128)

        low = tokens(at + odd)
        high = tokens(jnp.minimum(at + 2, TILES - 1)).astype(F32)
        if odd:
            high = pltpu.roll(high, 64, 1)
        return low, jnp.where(half_lane, high, 0.0)

    def prepare(f, odd):
        low, high = column_of(f, odd)
        x = jnp.concatenate([low, high.astype(BF16)], axis=1)
        rq[odd] = (mm(x, rwide[:, 0:256]) * QSCALE).astype(BF16)
        rkv = mm(x[0:KEYS], rwide[:, 256:768]).astype(BF16)
        for h in range(HEADS):
            at = 128 * (h // 4)
            rows = pl.ds(KEYS * h, KEYS)
            keys[odd, rows, :] = rkv[:, at : at + 128] * head_mask(h)
            vals[odd, rows, 0:128] = rkv[:, 256 + at : 384 + at] * head_mask(h)

    units = [(begin, first) for begin in range(0, ROWS, CHUNK) for first in (0, 2, 4)]

    def score_pair(odd, begin, first):
        at = 128 * (first // 4)
        return mm(rq[odd, begin : begin + CHUNK, at : at + 128], keys[odd, pl.ds(KEYS * first, 2 * KEYS), :], NT)

    def value_pair(odd, first, score):
        probs = []
        for i in range(2):
            s = score[:, KEYS * i : KEYS * i + KEYS] + rbias
            probs.append(jnp.exp2(s - jnp.max(s, axis=-1, keepdims=True)).astype(BF16))
        return mm(jnp.concatenate(probs, axis=1), vals[odd, pl.ds(KEYS * first, 2 * KEYS), :])

    def attend_rows(odd, fill=None):
        waiting = []
        got = None
        for n in range(len(units) + LAG):
            if n < len(units):
                waiting.append(score_pair(odd, *units[n]))
            if n == FILL and fill is not None:
                fill()
            if n >= LAG:
                begin, first = units[n - LAG]
                more = value_pair(odd, first, waiting.pop(0))
                got = more if first != 2 else got + more
                if first:
                    at = 128 * (first // 4)
                    ratt[odd, begin : begin + CHUNK, at : at + 128] = (got[:, :128] / got[:, 128:]).astype(BF16)

    def finish_column(f, odd):
        low, high = column_of(f, odd)
        mixed = mm(ratt[odd], rproj[...])
        low, high = layer_norm(low.astype(F32) + mixed[:, 0:128], high + mixed[:, 128:256])
        done[f, :, 0:32, :] = low.astype(BF16).reshape(PEERS, 32, 128)
        high = high.reshape(PEERS, 2, 16, 128)
        high = high[:, 0] + pltpu.roll(high[:, 1].reshape(PEERS * 16, 128), 64, 1).reshape(PEERS, 16, 128)
        done[f, :, 32:48, :] = high.astype(BF16)

    def send_column(f):
        def to_peer(k, _):
            p = lax.rem(me + k, PEERS)
            pass_on(done.at[f, p], normed.at[f, place(p)], k, "cells", p, send2_sem, recv2_sem.at[f])
            return 0

        lax.fori_loop(0, PEERS, to_peer, 0)

    pltpu.make_async_copy(cols.at[0], cols.at[0], cols_sem.at[4]).wait()
    arrive(0)
    prepare(0, 0)
    attend_rows(0, lambda: prepare(1, 1))

    def two_columns(g, _):
        f = 2 * g
        arrive(f)

        def fill():
            finish_column(f - 2, 0)
            prepare(f, 0)

        attend_rows(1, fill)
        send_column(f - 2)

        def fill_next():
            finish_column(f - 1, 1)

            prepare(jnp.minimum(f + 1, OWN - 2), 1)

        attend_rows(0, fill_next)
        send_column(f - 1)
        return 0

    lax.fori_loop(1, 4, two_columns, 0)
    finish_column(OWN - 1, 0)
    send_column(OWN - 1)

    def unpack(f, _):
        pltpu.make_async_copy(normed.at[f], normed.at[f], recv2_sem.at[f]).wait()
        for p in range(PEERS):
            at = pl.multiple_of((p * OWN + f) * STRIDE, 8)
            turn0[pl.ds(at, LOCAL), :] = normed[f, p, 0:32, :].astype(F32)
            high = normed[f, p, 32:48, :].astype(F32)
            turn1[pl.ds(at, 16), :] = high
            turn1[pl.ds(at + 16, 16), :] = pltpu.roll(high, 64, 1)
        return 0

    all_cot.wait()
    lax.fori_loop(0, OWN, unpack, 0)

    def feed(step, _):
        feed_forward(BLOCKS * step, cot_ref, turn0, turn1, win_t, wout, toks, acts, dcot, sums)
        return 0

    lax.fori_loop(0, STEPS // BLOCKS, feed, 0)

    def output(step, _):
        output_cells(step, wout_t, toks, acts, out_buf)
        rows = pl.ds(step * DROWS, DROWS)
        pltpu.make_async_copy(out_buf.at[rows], out_hbm.at[rows], local_sem.at[3]).start()
        return 0

    factor = 1.0 / math.sqrt(16 * ROWS * FEATS)
    part[0] = (sums[0, :, 0:128] * factor).astype(BF16)
    part[1] = (sums[1, :, 0:128] * (0.5 * factor)).astype(BF16)
    part[2, :, 0:64] = (sums[0, :, 128:192] * factor).astype(BF16)
    part[2, :, 64:128] = (sums[1, :, 128:192] * (0.5 * factor)).astype(BF16)

    table = lax.axis_index("tables") if remote else 0
    chip = me // 2
    core = me - 2 * chip
    theirs = pl.ds(pl.multiple_of((1 - core) * 384, 384), 384)
    mine = pl.ds(pl.multiple_of(core * 384, 384), 384)
    if remote:
        swap = pltpu.make_async_remote_copy(
            src_ref=part.at[:, theirs, :],
            dst_ref=pair,
            send_sem=sums_sem.at[0],
            recv_sem=sums_sem.at[1],
            device_id={"cells": 2 * chip + 1 - core},
            device_id_type=MESH,
        )
    else:
        swap = pltpu.make_async_copy(part.at[:, theirs, :], pair, sums_sem.at[1])
    swap.start()
    lax.fori_loop(0, STEPS // 8, output, 0)
    swap.wait()
    for t in range(3):
        half_sum[t] = (part[t, mine, :].astype(F32) + pair[t].astype(F32)).astype(BF16)

    def to_chip(k, _):
        p = lax.rem(chip + k, CHIPS)
        source = half_sum.at[:, pl.ds(pl.multiple_of(48 * p, 16), 48), :]
        target = got_chips.at[chip if remote else p]
        pass_on(source, target, k, "cells", 2 * p + core, sums_sem.at[2], sums_sem.at[3])
        return 0

    lax.fori_loop(0, CHIPS, to_chip, 0)
    lined[...] = jnp.zeros(lined.shape, F32)
    lax.fori_loop(STEPS // 8, STEPS * 5 // 8, output, 0)
    pltpu.make_async_copy(got_chips, got_chips, sums_sem.at[3]).wait()
    total = got_chips[0].astype(F32)
    for p in range(1, CHIPS):
        total = total + got_chips[p].astype(F32)
    for t in range(PEERS):
        for i in range(3):
            lined[t, 4 * i : 4 * i + 3, :] = total[i, 3 * t : 3 * t + 3, :]
    row[...] = lined[...].astype(BF16)

    def to_table(k, _):
        p = lax.rem(table + k, PEERS)
        pass_on(row.at[p], got_tables.at[table if remote else p], k, "tables", p, sums_sem.at[4], sums_sem.at[5])
        return 0

    lax.fori_loop(0, PEERS, to_table, 0)
    lax.fori_loop(STEPS * 5 // 8, STEPS, output, 0)
    if remote:
        sent = send.at[pl.ds(0, PEERS - 1)]
        pltpu.make_async_copy(sent, sent, send_sem).wait()
        sent = normed.at[:, pl.ds(0, PEERS - 1)]
        pltpu.make_async_copy(sent, sent, send2_sem).wait()
        sent = got_chips.at[pl.ds(0, CHIPS - 1)]
        pltpu.make_async_copy(sent, sent, sums_sem.at[2]).wait()
        sent = got_tables.at[pl.ds(0, PEERS - 1)]
        pltpu.make_async_copy(sent, sent, sums_sem.at[4]).wait()
    pltpu.make_async_copy(out_buf, out_hbm, local_sem.at[3]).wait()
    pltpu.make_async_copy(got_tables, got_tables, sums_sem.at[5]).wait()
    final = got_tables[0].astype(F32)
    for t in range(1, PEERS):
        final = final + got_tables[t].astype(F32)
    grad_in_ref[:, 0:128] = final[0:3, :]
    grad_in_ref[:, 128:192] = final[8:11, 0:64]
    grad_out_ref[:, 0:128] = final[4:7, :]
    grad_out_ref[:, 128:192] = final[8:11, 64:128]


def whole_layer(
    x_t, feat_count, train_count, feat_qkv, feat_proj, row_qkv, row_proj, w_in, w_out_t, cot_t, remote=True
):
    vmem = pl.BlockSpec(memory_space=pltpu.VMEM)
    smem = pl.BlockSpec(memory_space=pltpu.SMEM)
    hbm = pl.BlockSpec(memory_space=pl.ANY)
    return pl.pallas_call(
        functools.partial(layer_kernel, remote),
        name="layer",
        out_shape=(
            jax.ShapeDtypeStruct((LOCAL, E, FEATS), BF16),
            jax.ShapeDtypeStruct((3, E), F32),
            jax.ShapeDtypeStruct((3, E), F32),
        ),
        in_specs=[smem, smem] + [hbm] * 8,
        out_specs=(hbm, vmem, vmem),
        scratch_shapes=[
            pltpu.VMEM((256, 768), BF16),
            pltpu.VMEM((256, 256), BF16),
            pltpu.VMEM((256, 768), BF16),
            pltpu.VMEM((256, 256), BF16),
            pltpu.VMEM((FBLOCK * FEATS, 256), F32),
            pltpu.VMEM((FBLOCK * FEATS, 256), F32),
            pltpu.VMEM((FBLOCK * FEATS, 768), F32),
            pltpu.VMEM((FBLOCK, 512, 256), BF16),
            pltpu.VMEM((FBLOCK, 256, 256), BF16),
            pltpu.VMEM((FBLOCK * FEATS, 256), BF16),
            pltpu.VMEM((FEATS * STRIDE, 128), F32),
            pltpu.VMEM((FEATS * STRIDE, 128), F32),
            pltpu.VMEM((PEERS, 2, TILES, 16, 128), BF16),
            pltpu.VMEM((2, PEERS, TILES, 16, 128), BF16),
            pltpu.VMEM((2, ROWS, 256), BF16),
            pltpu.VMEM((2, HEADS * KEYS, 128), BF16),
            pltpu.VMEM((2, HEADS * KEYS, 256), BF16),
            pltpu.VMEM((2, ROWS, 256), BF16),
            pltpu.VMEM((OWN, PEERS, 48, 128), BF16),
            pltpu.VMEM((E, 3 * E), BF16),
            pltpu.VMEM((E, E), BF16),
            pltpu.VMEM((E, 3 * E), BF16),
            pltpu.VMEM((E, E), BF16),
            pltpu.VMEM((E, HID), BF16),
            pltpu.VMEM((E, HID), BF16),
            pltpu.VMEM((LOCAL, E, FEATS), BF16),
            pltpu.VMEM((LOCAL, E, FEATS), BF16),
            pltpu.VMEM((OWN, PEERS, 48, 128), BF16),
            pltpu.VMEM((HID, E), BF16),
            pltpu.VMEM((HID, E), BF16),
            pltpu.VMEM((E, HID), BF16),
            pltpu.VMEM((STEPS, DTOK, E), BF16),
            pltpu.VMEM((STEPS, HID, DTOK), BF16),
            pltpu.VMEM((BLOCKS, E, DTOK), BF16),
            pltpu.VMEM((2, HID, E), F32),
            pltpu.VMEM((LOCAL, E, FEATS), BF16),
            pltpu.VMEM((3, HID, 128), BF16),
            pltpu.VMEM((3, 384, 128), BF16),
            pltpu.VMEM((3, 384, 128), BF16),
            pltpu.VMEM((CHIPS, 3, 48, 128), BF16),
            pltpu.VMEM((PEERS, 16, 128), F32),
            pltpu.VMEM((PEERS, 16, 128), BF16),
            pltpu.VMEM((PEERS, 16, 128), BF16),
            pltpu.SemaphoreType.DMA,
            pltpu.SemaphoreType.DMA((5,)),
            pltpu.SemaphoreType.DMA,
            pltpu.SemaphoreType.DMA((OWN,)),
            pltpu.SemaphoreType.DMA((10,)),
            pltpu.SemaphoreType.DMA((6,)),
        ],
        compiler_params=pltpu.CompilerParams(
            collective_id=0 if remote else None, has_side_effects=True, vmem_limit_bytes=VMEM_LIMIT
        ),
    )(feat_count, train_count, x_t, feat_qkv, feat_proj, row_qkv, row_proj, w_in, w_out_t, cot_t)


PIECES = 8


def closing_kernel(cells_hbm, a_hbm, b_hbm, cells_out, a_out, b_out, cells, a, b, in_sem, out_sem):
    small = ((a_hbm, a, a_out), (b_hbm, b, b_out))
    size = LOCAL // PIECES
    steps = [(source, hold, target) for source, hold, target in small]
    steps += [tuple(ref.at[pl.ds(size * i, size)] for ref in (cells_hbm, cells, cells_out)) for i in range(PIECES)]
    loads = [pltpu.make_async_copy(source, hold, in_sem.at[i]) for i, (source, hold, _) in enumerate(steps)]
    stores = [pltpu.make_async_copy(hold, target, out_sem.at[i]) for i, (_, hold, target) in enumerate(steps)]
    for copy in loads:
        copy.start()
    for load, store in zip(loads, stores):
        load.wait()
        store.start()
    for copy in stores:
        copy.wait()


def close(cells, a, b):
    hbm = pl.BlockSpec(memory_space=pl.ANY)
    return pl.pallas_call(
        closing_kernel,
        name="closing_copies",
        out_shape=tuple(jax.ShapeDtypeStruct(v.shape, v.dtype) for v in (cells, a, b)),
        in_specs=[hbm] * 3,
        out_specs=(hbm,) * 3,
        scratch_shapes=[pltpu.VMEM(v.shape, v.dtype) for v in (cells, a, b)]
        + [pltpu.SemaphoreType.DMA((PIECES + 2,)), pltpu.SemaphoreType.DMA((PIECES + 2,))],
        compiler_params=pltpu.CompilerParams(vmem_limit_bytes=VMEM_LIMIT),
    )(cells, a, b)


def per_device(
    cells_in, train_count, feat_count, feat_qkv, feat_proj, row_qkv, row_proj, w_in, w_out, cotangent
):
    x_t = jnp.swapaxes(cells_in[0], 1, 2)
    cot_t = jnp.swapaxes(cotangent[0], 1, 2)
    out_t, grad_in, grad_out = whole_layer(
        x_t, feat_count, train_count, feat_qkv, feat_proj, row_qkv, row_proj, w_in, w_out.T, cot_t
    )
    out_t, grad_in, grad_out = close(out_t, grad_in, grad_out)
    return (jnp.swapaxes(out_t, 1, 2)[None], grad_in.T, grad_out)


def solution(mesh):
    return jax.shard_map(
        per_device,
        mesh=mesh,
        in_specs=(
            P("tables", "cells", None, None),
            P("tables"),
            P("tables"),
            P(),
            P(),
            P(),
            P(),
            P(),
            P(),
            P("tables", "cells", None, None),
        ),
        out_specs=(
            P("tables", "cells", None, None),
            P(None, ("tables", "cells")),
            P(("tables", "cells"), None),
        ),
        check_vma=False,
    )
```
